512 devices in a mesh: elem: 64 (over y, x, core), node: 8 (over z).
Axes of the slice: x: 4, y: 8, z: 8, core: 2. Of those that a mesh axis runs over, the one named last changes fastest.
Arguments:
- factors: bfloat16 [12, 12, 524288], P(None, None, ('elem', 'node')), may hold values from -0.3984375 to 0.3984375
- dest_device: int32 [524288, 1], P(('elem', 'node')), may hold values from 0 to 511; in each aligned block of 1024 rows (0 to 1023, 1024 to 2047, ...) at most 3 rows name the same one
- dest_node: int32 [524288, 1], P(('elem', 'node')), may hold values from 0 to 15
- live_count: int32 [512], P(('elem', 'node')), may hold values from 768 to 1024, as said below
- shift: float32 [12, 8192], P(None, ('elem', 'node')), may hold values from 0.3 to 3
Outputs:
- inverse: float32 [12, 12, 8192], P(None, None, ('elem', 'node'))
The draws below stay inside these ranges and needn't reach their ends.
Inputs may be any that keep to these rules, and one draw needn't show every extreme that they name: A device's live contributions are its first live_count ones; on some devices all 1024 are live. `dest_device`: among the 1024 contributions of one device, at most 3 name the same owner.
All inputs are finite; a program needn't handle non-finite values.
Results may differ from the reference program's by a relative error of at most 0.0003.
Values sent between devices are 32-bit elements; how exact they have to be, the bound alone decides.
A program may use at most 64 MiB of HBM per device.

```python
import math
import jax
import jax.numpy as jnp
import numpy as np
from jax import lax

BLOCK = 12
C_DEV = 1024
NODE_DEV = 16
CAP = 3
CONTRIB = 524288
NODES = 8192
DEVICES = 512


def draw_live_count(key, part):
    first_key = jax.random.fold_in(key, 11)
    second_key = jax.random.fold_in(key, 23)
    base = jax.random.randint(first_key, (DEVICES,), 3 * C_DEV // 4, C_DEV + 1)
    order = jax.random.permutation(second_key, DEVICES)
    chosen = order[:max(1, DEVICES // 16)]
    base = base.at[chosen].set(C_DEV)
    return base.astype(jnp.int32)


def with_ends(values, stream_key, smallest, high):
    longest = values.shape.index(max(values.shape))
    spots = []
    for shift in (0, 1):
        where = [jax.random.randint(jax.random.fold_in(stream_key, axis), (), 0, length) for axis, length in enumerate(values.shape)]
        where[longest] = (where[longest] + shift) % values.shape[longest]
        spots.append(tuple(where))
    return values.at[spots[0]].set(smallest).at[spots[1]].set(high)


def steps_of(own_key, extent, pieces, smallest, largest):
    def one(dim, blocks):
        draws = jax.random.uniform(jax.random.fold_in(jax.random.fold_in(own_key, 6), dim), (blocks,), jnp.float32, smallest / len(pieces), largest / len(pieces))
        return jnp.repeat(jnp.exp(draws), extent[dim] // blocks).reshape((-1,) + (1,) * (len(extent) - dim - 1))

    factor_of = one(*pieces[0])
    for cut in pieces[1:]:
        factor_of = factor_of * one(*cut)
    return factor_of


def assign_block(rng, own, number, rows, count, top, reach, skew):
    ranking = jax.random.permutation(rng, count)
    crowded, ordinary = shares(count, rows * top, reach, skew, True), shares(count, rows * top, reach, skew, False)
    places = jnp.arange(count)

    def named(lengths, offset_by):
        used = int((lengths > 0).sum())
        fixed = max(1, used // 4)
        shifted = fixed + (places - fixed + offset_by * (used - fixed)) % max(1, count - fixed)
        return jnp.zeros((count,), jnp.int32).at[ranking[jnp.where(places < fixed, places, shifted)]].set(jnp.asarray(lengths, jnp.int32))

    lengths = jnp.where(number % 4 == 0, named(crowded, number // 4), named(ordinary, number - number // 4 - 1))
    mixed = jax.random.permutation(jax.random.fold_in(own, 3), count)
    giver, sink = mixed[0:count // 2 * 2:2], mixed[1:count // 2 * 2:2]
    margin = jnp.minimum(lengths[giver] - 1, reach - lengths[sink]) // 2
    margin = jnp.where((giver == ranking[0]) | (sink == ranking[0]) | (lengths[sink] == 0), 0, jnp.maximum(margin, 0))
    shifted = jax.random.randint(jax.random.fold_in(own, 4), (count // 2,), 0, 1 << 20) % (margin + 1)
    lengths = lengths.at[giver].add(-shifted).at[sink].add(shifted)
    members = jnp.searchsorted(jnp.cumsum(lengths), jnp.arange(rows * top), side="right").astype(jnp.int32)
    listing = members.reshape(top, rows).T
    listing = listing[jax.random.permutation(jax.random.fold_in(own, 1), rows)]
    offset_by = jax.random.randint(jax.random.fold_in(own, 2), (rows, 1), 0, top)
    return jnp.take_along_axis(listing, (jnp.arange(top)[None, :] + offset_by) % top, axis=1)


def shares(count, total, reach, slope, full):
    loads = [(1 << 20) // math.isqrt(grade ** slope) + 1 for grade in range(1, count + 1)]
    largest = reach if full else min(reach, max(-(-total // count), total * loads[0] // sum(loads)))
    least = 1 if total - largest >= count - 1 else 0
    holding, spare = [largest] + [least] * (count - 1), total - largest - least * (count - 1)
    while spare > 0:
        candidates = [i for i in range(1, count) if holding[i] < largest] or [i for i in range(1, count) if holding[i] < reach]
        mass, remaining = sum([loads[i] for i in candidates]), spare
        for i in candidates:
            more = min(reach - holding[i], max(1, remaining * loads[i] // mass), spare)
            holding[i] = holding[i] + more
            spare = spare - more
    return np.array(holding)


def normal_values(key, extent, width, limit, cuts=(), kind=jnp.bfloat16):
    values = jax.random.normal(key, extent, jnp.float32) * width
    if len(cuts) > 0:
        values = steps_of(key, extent, cuts, -0.22, 0.18) * values
    return jnp.clip(values, min=-limit, max=limit).astype(kind)


def setup_inputs(seed: int = 0) -> dict:
    splits = jax.random.split(jax.random.key(seed), 6)
    factors = normal_values(splits[0], (BLOCK, BLOCK, CONTRIB), 0.06, 0.3984375, ((2, 512),))
    dest_device_keys = jax.random.split(jax.random.fold_in(splits[1], 1), CONTRIB // C_DEV)
    dest_device_turns = jax.random.permutation(jax.random.fold_in(splits[1], 3), CONTRIB // C_DEV)
    dest_device = jax.vmap(lambda own, number: assign_block(jax.random.fold_in(splits[1], 2), own, number, C_DEV, DEVICES, 1, CAP, 1))(dest_device_keys, dest_device_turns).reshape((CONTRIB, 1))
    dest_node = with_ends(jax.random.randint(splits[2], (CONTRIB, 1), 0, NODE_DEV), jax.random.fold_in(splits[2], 1), 0, NODE_DEV - 1).astype(jnp.int32)
    live_count = draw_live_count(jax.random.fold_in(splits[5], 71), 0)
    shift = jnp.clip(jnp.exp(math.log(3.0) - 2.3025851 * jax.random.uniform(splits[4], (BLOCK, NODES), jnp.float32) ** steps_of(splits[4], (BLOCK, NODES), ((1, 512),), -0.2, 0.2)), 0.3, 3.0)
    return dict(factors=factors, dest_device=dest_device, dest_node=dest_node, live_count=live_count, shift=shift)


def block_inverse(matrix):
    size = matrix.shape[0]
    lower = [[None] * size for _ in range(size)]
    for column in range(size):
        total = matrix[column, column]
        for inner in range(column):
            total = total - lower[column][inner] * lower[column][inner]
        pivot = jnp.sqrt(total)
        lower[column][column] = pivot
        for target in range(column + 1, size):
            total = matrix[target, column]
            for inner in range(column):
                total = total - lower[target][inner] * lower[column][inner]
            lower[target][column] = total / pivot
    solved = [[None] * size for _ in range(size)]
    for target in range(size):
        solved[target][target] = 1.0 / lower[target][target]
        for column in range(target):
            total = lower[target][column] * solved[column][column]
            for inner in range(column + 1, target):
                total = total + lower[target][inner] * solved[inner][column]
            solved[target][column] = -total / lower[target][target]
    rows_out = []
    for first in range(size):
        entries = []
        for second in range(size):
            total = solved[max(first, second)][first] * solved[max(first, second)][second]
            for inner in range(max(first, second) + 1, size):
                total = total + solved[inner][first] * solved[inner][second]
            entries.append(total)
        rows_out.append(jnp.stack(entries))
    return jnp.stack(rows_out)

def reference(factors, dest_device, dest_node, live_count, shift):

    def accumulate(acc, device):
        start = (device * C_DEV).astype(jnp.int32)
        piece = lax.dynamic_slice_in_dim(factors, start, C_DEV, 2).astype(jnp.float32)
        contrib = jnp.einsum('akc,bkc->abc', piece, piece, precision=lax.Precision.HIGHEST)
        contrib = contrib.reshape(BLOCK * BLOCK, C_DEV)
        owners = lax.dynamic_slice_in_dim(dest_device[:, 0], start, C_DEV, 0)
        places = lax.dynamic_slice_in_dim(dest_node[:, 0], start, C_DEV, 0)
        alive = jnp.arange(C_DEV, dtype=jnp.int32) < live_count[device]
        targets = jnp.where(alive, owners * NODE_DEV + places, NODES).astype(jnp.int32)
        acc = acc.at[targets].add(contrib.T, mode='drop')
        return (acc, None)
    start_acc = jnp.zeros((NODES, BLOCK * BLOCK), jnp.float32)
    summed, unused = lax.scan(accumulate, start_acc, jnp.arange(DEVICES, dtype=jnp.int32))
    assembled = summed.T.reshape(BLOCK, BLOCK, NODES)
    identity = jnp.eye(BLOCK, dtype=jnp.float32)
    matrix = assembled + identity[:, :, None] * shift[:, None, :]
    return block_inverse(matrix)
```

```python
import functools

import jax
import jax.numpy as jnp
from jax import lax
from jax.experimental import pallas as pl
from jax.experimental.pallas import tpu as pltpu
from jax.sharding import PartitionSpec as P

MESH = pl.DeviceIdType.MESH
F32 = jnp.float32
BF16 = jnp.bfloat16
SIZE = 12
COUNT = 1024
NODES = 16
NX, NY, NZ, NC = 4, 8, 8, 2
OFFSET = [a * SIZE - a * (a - 1) // 2 for a in range(SIZE)]
ROWS = 80
MESSAGE = 120


def lanes(shape):
    return lax.broadcasted_iota(jnp.int32, shape, len(shape) - 1)


def ranks_of(owner):
    counts = [jnp.zeros((8, 128), F32) for _ in range(8)]
    rows = [owner[:, b * 128 : (b + 1) * 128] for b in range(8)]
    before = lax.broadcasted_iota(jnp.int32, (128, 128), 0) < lanes((128, 128))
    for b in range(8):
        column = jnp.broadcast_to(rows[b], (128, 128)).T
        for later in range(b, 8):
            same = column == rows[later]
            if later == b:
                same = same & before
            hits = jnp.where(same, 1.0, 0.0)
            counts[later] = counts[later] + jnp.sum(hits.reshape(16, 8, 128), axis=0)
    return jnp.concatenate([jnp.sum(c, axis=0, keepdims=True) for c in counts], axis=1)


def exchange_kernel(
    factors,
    owner_ref,
    node_ref,
    live_ref,
    out,
    lhs,
    routed,
    packed,
    send1,
    recv1,
    dense,
    recv2,
    send3,
    recv3,
    ssem1,
    rsem1,
    ssem2,
    rsem2,
    ssem3,
    rsem3,
):
    elem = lax.axis_index("elem")
    z = lax.axis_index("node")
    core = lax.rem(elem, NC)
    x = lax.rem(elem // NC, NX)
    y = elem // (NC * NX)

    def device(y_at, x_at, core_at, z_at):
        return ((y_at * NX + x_at) * NC + core_at, z_at)

    def partner1(i):
        return device(y, lax.rem(x + i // 2, NX), lax.rem(core + i, NC), z)

    def partner2(i):
        return device(lax.rem(y + i * (1 - core), NY), x, core, lax.rem(z + i * core, NZ))

    def partner3(i):
        return device(lax.rem(y + i * core, NY), x, core, lax.rem(z + i * (1 - core), NZ))

    barrier = pltpu.get_barrier_semaphore()
    for partner in (partner1, partner2, partner3):
        for i in range(1, 8):
            pl.semaphore_signal(barrier, inc=1, device_id=partner(i), device_id_type=MESH)

    first = y * (1 - core) + z * core
    second = z * (1 - core) + y * core

    for a in range(SIZE):
        lhs[a * 16 : a * 16 + SIZE, :] = factors[a]
    lhs[192:208, :] = jnp.broadcast_to(node_ref[...].astype(F32), (16, COUNT)).astype(BF16)

    owner = owner_ref[...]
    rank = ranks_of(owner.astype(F32)).astype(jnp.int32)
    owner_z = owner & 7
    owner_core = (owner >> 3) & 1
    owner_x = (owner >> 4) & 3
    owner_y = owner >> 6
    other = owner_core ^ core
    step = (owner_x - x + NX) & 3
    slot = jnp.where(rank < 2, other * 128 + rank * 64, 256 + other * 64)
    slot = slot + step * 384 + owner_y * 8 + owner_z
    slot = jnp.where(lanes((1, COUNT)) < live_ref[0], slot, -1)

    low = lanes((40, 128)) < 64

    def prepare(step):
        wanted = lax.broadcasted_iota(jnp.int32, (384, COUNT), 0)
        choice = jnp.where(wanted == slot - step * 384, 1.0, 0.0).astype(BF16)
        result = lax.dot_general(
            lhs[...], choice, (((1,), (1,)), ((), ())), preferred_element_type=F32
        )
        for t in range(3):
            routed[t] = result[:, t * 128 : (t + 1) * 128]

        def product(t, carry):
            total = [None] * SIZE
            for k in range(SIZE):
                column = routed[t, pl.ds(k, SIZE, stride=16), :]
                for a in range(SIZE):
                    term = routed[t, a * 16 + k : a * 16 + k + 1, :] * column
                    total[a] = term if k == 0 else total[a] + term
            for a in range(SIZE):
                packed[t, OFFSET[a] : OFFSET[a] + SIZE - a, :] = total[a][a:SIZE]
            packed[t, 78:80, :] = routed[t, 192:194, :]
            return carry

        lax.fori_loop(0, 3, product, 0)
        upper, bottom = packed[2, 0:40, :], packed[2, 40:80, :]
        first_half = jnp.where(low, upper, pltpu.roll(bottom, 64, 1))
        second_half = jnp.where(low, pltpu.roll(upper, 64, 1), bottom)
        return first_half, second_half

    def fill(target, index, part, half):
        target[index, 0:ROWS, :] = packed[part]
        target[index, ROWS:MESSAGE, :] = half

    def copy1(i):
        return pltpu.make_async_remote_copy(
            src_ref=send1.at[i],
            dst_ref=recv1.at[i],
            send_sem=ssem1.at[i],
            recv_sem=rsem1.at[i],
            device_id=partner1(i),
            device_id_type=MESH,
        )

    pl.semaphore_wait(barrier, 21)

    def pair(step, carry):
        first_half, second_half = prepare(step)
        fill(send1, 2 * step, 0, first_half)
        fill(send1, 2 * step + 1, 1, second_half)
        copy1(2 * step).start()
        copy1(2 * step + 1).start()
        return carry

    lax.fori_loop(1, NX, pair, 0)
    first_half, second_half = prepare(0)
    fill(send1, 1, 1, second_half)
    copy1(1).start()
    fill(recv1, 0, 0, first_half)

    lane = lanes((1, 256)) & 63
    lane_y, lane_z = lane >> 3, lane & 7
    base = (lane_y * (1 - core) + lane_z * core) * 128
    base = base + (lane_z * (1 - core) + lane_y * core) * 16
    low_row = lanes((1, 128)) < 64

    def gather(i):
        top = recv1[i, 0:ROWS, :]
        half = recv1[i, ROWS:MESSAGE, :]
        ids_half = recv1[i, ROWS + 38 : ROWS + 39, :]
        ids = jnp.concatenate(
            [recv1[i, 78:79, :], jnp.where(low_row, pltpu.roll(ids_half, 64, 1), ids_half)], axis=1
        )
        place = base + ids.astype(jnp.int32)
        spread = jnp.concatenate([jnp.where(low, half, 0.0), jnp.where(low, 0.0, half)], axis=0)
        values = jnp.concatenate([top, spread], axis=1)
        high = values.astype(BF16)
        rest = values - high.astype(F32)
        middle = rest.astype(BF16)
        tail = (rest - middle.astype(F32)).astype(BF16)
        pieces = jnp.concatenate([high, middle, tail], axis=0)
        for part in range(4):
            wanted = lax.broadcasted_iota(jnp.int32, (256, 256), 0) + part * 256
            choice = jnp.where(wanted == place, 1.0, 0.0).astype(BF16)
            found = lax.dot_general(
                pieces, choice, (((1,), (1,)), ((), ())), preferred_element_type=F32
            )
            found = found[0:ROWS] + found[ROWS : 2 * ROWS] + found[2 * ROWS : 3 * ROWS]
            yield part, found

    for part, found in gather(0):
        dense[2 * part] = found[:, 0:128]
        dense[2 * part + 1] = found[:, 128:256]

    def absorb(i, carry):
        copy1(i).wait_recv()
        for part, found in gather(i):
            dense[2 * part] = dense[2 * part] + found[:, 0:128]
            dense[2 * part + 1] = dense[2 * part + 1] + found[:, 128:256]
        return carry

    lax.fori_loop(1, 8, absorb, 0)

    def copy2(i):
        return pltpu.make_async_remote_copy(
            src_ref=dense.at[lax.rem(first + i, 8)],
            dst_ref=recv2.at[i],
            send_sem=ssem2.at[i],
            recv_sem=rsem2.at[i],
            device_id=partner2(i),
            device_id_type=MESH,
        )

    for i in (4, 3, 5, 2, 6, 1, 7):
        copy2(i).start()
    total = dense[first]
    for i in (1, 7, 2, 6, 3, 5, 4):
        copy2(i).wait_recv()
        total = total + recv2[i]

    lane_full = lanes((8, 128))

    def swap(tiles):
        for span in (4, 2, 1):
            width = span * 16
            lower = (lane_full & width) == 0
            result = list(tiles)
            for v in range(8):
                if v & span:
                    continue
                one, two = tiles[v], tiles[v + span]
                result[v] = jnp.where(lower, one, pltpu.roll(two, width, 1))
                result[v + span] = jnp.where(lower, pltpu.roll(one, 128 - width, 1), two)
            tiles = result
        return tiles

    rows = [total[v * 8 : v * 8 + 8] for v in range(10)]
    empty = jnp.zeros((8, 128), F32)
    main = swap(rows[0:8])
    extra = swap(rows[8:10] + [empty] * 6)
    for q in range(8):
        send3[q, 0:8, :] = main[q]
        send3[q, 8:16, :] = extra[q]

    def copy3(i):
        return pltpu.make_async_remote_copy(
            src_ref=send3.at[lax.rem(second + i, 8)],
            dst_ref=recv3.at[i],
            send_sem=ssem3.at[i],
            recv_sem=rsem3.at[i],
            device_id=partner3(i),
            device_id_type=MESH,
        )

    for i in (4, 3, 5, 2, 6, 1, 7):
        copy3(i).start()
    result = send3[second]
    for i in (1, 7, 2, 6, 3, 5, 4):
        copy3(i).wait_recv()
        result = result + recv3[i]
    out[...] = result
    for i in range(1, 8):
        copy1(i).wait_send()
        copy2(i).wait_send()
        copy3(i).wait_send()


def inverse_kernel(sums, shift, out, flat, square):
    for v in range(10):
        source = sums[0:8, :] if v < 8 else sums[8:16, :]
        turned = 16 * v % 128
        flat[v * 8 : v * 8 + 8, :] = pltpu.roll(source, 128 - turned, 1) if turned else source
    for j in range(SIZE):
        square[j, j:SIZE, :] = flat[OFFSET[j] : OFFSET[j] + SIZE - j, 0:NODES]
        for i in range(j):
            place = OFFSET[i] + j - i
            square[j, i : i + 1, :] = flat[place : place + 1, 0:NODES]
    row = lax.broadcasted_iota(jnp.int32, (SIZE, NODES), 0)
    columns = []
    for j in range(SIZE):
        added = jnp.where(row == j, shift[j : j + 1, :], 0.0)
        columns.append(square[j] + added)
    for j in range(SIZE):
        current = columns[j]
        here = row == j
        scale = 1.0 / current[j : j + 1, :]
        scaled = jnp.where(here, -scale, current * scale)
        for k in range(SIZE):
            if k == j:
                continue
            kept = jnp.where(here, 0.0, columns[k])
            columns[k] = kept - scaled * current[k : k + 1, :]
        columns[j] = scaled
    for j in range(SIZE):
        out[j] = -columns[j]


def shards(factors, dest_device, dest_node, live_count, shift):
    vmem = pl.BlockSpec(memory_space=pltpu.VMEM)
    sums = pl.pallas_call(
        exchange_kernel,
        out_shape=jax.ShapeDtypeStruct((16, 128), F32),
        in_specs=[vmem, vmem, vmem, pl.BlockSpec(memory_space=pltpu.SMEM)],
        out_specs=vmem,
        scratch_shapes=[
            pltpu.VMEM((208, COUNT), BF16),
            pltpu.VMEM((3, 208, 128), F32),
            pltpu.VMEM((3, ROWS, 128), F32),
            pltpu.VMEM((8, MESSAGE, 128), F32),
            pltpu.VMEM((8, MESSAGE, 128), F32),
            pltpu.VMEM((8, ROWS, 128), F32),
            pltpu.VMEM((8, ROWS, 128), F32),
            pltpu.VMEM((8, 16, 128), F32),
            pltpu.VMEM((8, 16, 128), F32),
        ]
        + [pltpu.SemaphoreType.DMA((8,))] * 6,
        compiler_params=pltpu.CompilerParams(collective_id=0, has_side_effects=True),
    )(factors, dest_device.reshape(1, COUNT), dest_node.reshape(1, COUNT), live_count)
    return pl.pallas_call(
        inverse_kernel,
        out_shape=jax.ShapeDtypeStruct((SIZE, SIZE, NODES), F32),
        in_specs=[vmem, vmem],
        out_specs=vmem,
        scratch_shapes=[pltpu.VMEM((ROWS, 128), F32), pltpu.VMEM((SIZE, SIZE, NODES), F32)],
    )(sums, shift)


def solution(mesh):
    placed = (
        P(None, None, ("elem", "node")),
        P(("elem", "node"), None),
        P(("elem", "node"), None),
        P(("elem", "node")),
        P(None, ("elem", "node")),
    )
    return jax.shard_map(
        shards,
        mesh=mesh,
        in_specs=placed,
        out_specs=P(None, None, ("elem", "node")),
        check_vma=False,
    )
```

```python
import functools

import jax
import jax.numpy as jnp
from jax import lax
from jax.experimental import pallas as pl
from jax.experimental.pallas import tpu as pltpu
from jax.sharding import PartitionSpec as P

MESH = pl.DeviceIdType.MESH
F32 = jnp.float32
BF16 = jnp.bfloat16
SIZE = 12
COUNT = 1024
NODES = 16
NX, NY, NZ, NC = 4, 8, 8, 2
OFFSET = [a * SIZE - a * (a - 1) // 2 for a in range(SIZE)]
ROWS = 80
MESSAGE = 120


def lanes(shape):
    return lax.broadcasted_iota(jnp.int32, shape, len(shape) - 1)


def ranks_of(owner):
    counts = [jnp.zeros((8, 128), F32) for _ in range(8)]
    rows = [owner[:, b * 128 : (b + 1) * 128] for b in range(8)]
    before = lax.broadcasted_iota(jnp.int32, (128, 128), 0) < lanes((128, 128))
    for b in range(8):
        column = jnp.broadcast_to(rows[b], (128, 128)).T
        for later in range(b, 8):
            same = column == rows[later]
            if later == b:
                same = same & before
            hits = jnp.where(same, 1.0, 0.0)
            counts[later] = counts[later] + jnp.sum(hits.reshape(16, 8, 128), axis=0)
    return jnp.concatenate([jnp.sum(c, axis=0, keepdims=True) for c in counts], axis=1)


def exchange_kernel(
    factors_in,
    owner_in,
    node_in,
    live_ref,
    out,
    factors,
    owner_ref,
    node_ref,
    isem,
    lhs,
    routed,
    packed,
    send1,
    recv1,
    dense,
    recv2,
    send3,
    recv3,
    ssem1,
    rsem1,
    ssem2,
    rsem2,
    ssem3,
    rsem3,
):
    inputs = [
        pltpu.make_async_copy(source, target, isem.at[n])
        for n, (source, target) in enumerate(
            [(owner_in, owner_ref), (node_in, node_ref), (factors_in, factors)]
        )
    ]
    for copy in inputs:
        copy.start()
    elem = lax.axis_index("elem")
    z = lax.axis_index("node")
    core = lax.rem(elem, NC)
    x = lax.rem(elem // NC, NX)
    y = elem // (NC * NX)

    def device(y_at, x_at, core_at, z_at):
        return ((y_at * NX + x_at) * NC + core_at, z_at)

    def partner1(i):
        return device(y, lax.rem(x + i // 2, NX), lax.rem(core + i, NC), z)

    def partner2(i):
        return device(lax.rem(y + i * (1 - core), NY), x, core, lax.rem(z + i * core, NZ))

    def partner3(i):
        return device(lax.rem(y + i * core, NY), x, core, lax.rem(z + i * (1 - core), NZ))

    barrier = pltpu.get_barrier_semaphore()
    for partner in (partner1, partner2, partner3):
        for i in range(1, 8):
            pl.semaphore_signal(barrier, inc=1, device_id=partner(i), device_id_type=MESH)

    first = y * (1 - core) + z * core
    second = z * (1 - core) + y * core

    inputs[0].wait()
    owner = owner_ref[...]
    rank = ranks_of(owner.astype(F32)).astype(jnp.int32)
    owner_z = owner & 7
    owner_core = (owner >> 3) & 1
    owner_x = (owner >> 4) & 3
    owner_y = owner >> 6
    other = owner_core ^ core
    step = (owner_x - x + NX) & 3
    slot = jnp.where(rank < 2, other * 128 + rank * 64, 256 + other * 64)
    outer = owner_y * (1 - owner_core) + owner_z * owner_core
    inner = owner_z * (1 - owner_core) + owner_y * owner_core
    lane = (outer * 8 + inner + ((2 * step + other) & 3) * 16) & 63
    slot = slot + step * 384 + lane
    slot = jnp.where(lanes((1, COUNT)) < live_ref[0], slot, -1)

    inputs[1].wait()
    inputs[2].wait()
    for a in range(SIZE):
        lhs[a * 16 : a * 16 + SIZE, :] = factors[a]
    lhs[192:208, :] = jnp.broadcast_to(node_ref[...].astype(F32), (16, COUNT)).astype(BF16)

    low = lanes((40, 128)) < 64

    def prepare(step):
        wanted = lax.broadcasted_iota(jnp.int32, (384, COUNT), 0)
        choice = jnp.where(wanted == slot - step * 384, 1.0, 0.0).astype(BF16)
        result = lax.dot_general(
            lhs[...], choice, (((1,), (1,)), ((), ())), preferred_element_type=F32
        )
        for t in range(3):
            routed[t] = result[:, t * 128 : (t + 1) * 128]

        def product(t, carry):
            total = [None] * SIZE
            for k in range(SIZE):
                column = routed[t, pl.ds(k, SIZE, stride=16), :]
                for a in range(SIZE):
                    term = routed[t, a * 16 + k : a * 16 + k + 1, :] * column
                    total[a] = term if k == 0 else total[a] + term
            for a in range(SIZE):
                packed[t, OFFSET[a] : OFFSET[a] + SIZE - a, :] = total[a][a:SIZE]
            packed[t, 78:80, :] = routed[t, 192:194, :]
            return carry

        lax.fori_loop(0, 3, product, 0)
        upper, bottom = packed[2, 0:40, :], packed[2, 40:80, :]
        first_half = jnp.where(low, upper, pltpu.roll(bottom, 64, 1))
        second_half = jnp.where(low, pltpu.roll(upper, 64, 1), bottom)
        return first_half, second_half

    def fill(target, index, part, half):
        target[index, 0:ROWS, :] = packed[part]
        target[index, ROWS:MESSAGE, :] = half

    def copy1(i):
        return pltpu.make_async_remote_copy(
            src_ref=send1.at[i],
            dst_ref=recv1.at[i],
            send_sem=ssem1.at[i],
            recv_sem=rsem1.at[i],
            device_id=partner1(i),
            device_id_type=MESH,
        )

    def send(step):
        first_half, second_half = prepare(step)
        fill(send1, 2 * step, 0, first_half)
        fill(send1, 2 * step + 1, 1, second_half)

    def start(step):
        copy1(2 * step).start()
        copy1(2 * step + 1).start()

    send(2)
    pl.semaphore_wait(barrier, 21)
    start(2)

    def pair(turn, carry):
        step = 1 + 2 * turn
        send(step)
        start(step)
        return carry

    lax.fori_loop(0, 2, pair, 0)
    first_half, second_half = prepare(0)
    fill(send1, 1, 1, second_half)
    copy1(1).start()
    fill(recv1, 0, 0, first_half)

    base = (lanes((1, 256)) & 15) * 16
    block = (lanes((1, 256)) & 63) >> 4
    low_row = lanes((1, 128)) < 64
    wanted = lax.broadcasted_iota(jnp.int32, (256, 256), 0)

    def batch(begin):
        for part in range(4):
            values = ids = None
            for source in range(4):
                i = begin + source
                half = recv1[i, ROWS:MESSAGE, :]
                spread = jnp.concatenate(
                    [jnp.where(low, half, 0.0), jnp.where(low, 0.0, half)], axis=0
                )
                value = jnp.concatenate([recv1[i, 0:ROWS, :], spread], axis=1)
                ids_half = recv1[i, ROWS + 38 : ROWS + 39, :]
                ids_half = jnp.where(low_row, pltpu.roll(ids_half, 64, 1), ids_half)
                ident = jnp.concatenate([recv1[i, 78:79, :], ids_half], axis=1)
                here = block == (part + source) % 4
                values = value if source == 0 else jnp.where(here, value, values)
                ids = ident if source == 0 else jnp.where(here, ident, ids)
            place = base + ids.astype(jnp.int32)
            high = values.astype(BF16)
            rest = values - high.astype(F32)
            middle = rest.astype(BF16)
            tail = (rest - middle.astype(F32)).astype(BF16)
            pieces = jnp.concatenate([high, middle, tail], axis=0)
            choice = jnp.where(wanted == place, 1.0, 0.0).astype(BF16)
            found = lax.dot_general(
                pieces, choice, (((1,), (1,)), ((), ())), preferred_element_type=F32
            )
            found = found[0:ROWS] + found[ROWS : 2 * ROWS] + found[2 * ROWS : 3 * ROWS]
            for side in range(2):
                piece = found[:, side * 128 : side * 128 + 128]
                if begin:
                    piece = dense[2 * part + side] + piece
                dense[2 * part + side] = piece

    for i in (1, 2, 3):
        copy1(i).wait_recv()
    batch(0)
    for i in (6, 7, 4, 5):
        copy1(i).wait_recv()
    batch(4)

    def copy2(i):
        return pltpu.make_async_remote_copy(
            src_ref=dense.at[lax.rem(first + i, 8)],
            dst_ref=recv2.at[i],
            send_sem=ssem2.at[i],
            recv_sem=rsem2.at[i],
            device_id=partner2(i),
            device_id_type=MESH,
        )

    for i in (4, 3, 5, 2, 6, 1, 7):
        copy2(i).start()
    total = dense[first]
    for i in (1, 7, 2, 6, 3, 5, 4):
        copy2(i).wait_recv()
        total = total + recv2[i]

    lane_full = lanes((8, 128))

    def swap(tiles):
        for span in (4, 2, 1):
            width = span * 16
            lower = (lane_full & width) == 0
            result = list(tiles)
            for v in range(8):
                if v & span:
                    continue
                one, two = tiles[v], tiles[v + span]
                result[v] = jnp.where(lower, one, pltpu.roll(two, width, 1))
                result[v + span] = jnp.where(lower, pltpu.roll(one, 128 - width, 1), two)
            tiles = result
        return tiles

    rows = [total[v * 8 : v * 8 + 8] for v in range(10)]
    empty = jnp.zeros((8, 128), F32)
    main = swap(rows[0:8])
    extra = swap(rows[8:10] + [empty] * 6)
    for q in range(8):
        send3[q, 0:8, :] = main[q]
        send3[q, 8:16, :] = extra[q]

    def copy3(i):
        return pltpu.make_async_remote_copy(
            src_ref=send3.at[lax.rem(second + i, 8)],
            dst_ref=recv3.at[i],
            send_sem=ssem3.at[i],
            recv_sem=rsem3.at[i],
            device_id=partner3(i),
            device_id_type=MESH,
        )

    for i in (4, 3, 5, 2, 6, 1, 7):
        copy3(i).start()
    result = send3[second]
    for i in (1, 7, 2, 6, 3, 5, 4):
        copy3(i).wait_recv()
        result = result + recv3[i]
    out[...] = result
    for i in range(1, 8):
        copy1(i).wait_send()
        copy2(i).wait_send()
        copy3(i).wait_send()


def inverse_kernel(sums, shift, out, flat, square):
    for v in range(10):
        source = sums[0:8, :] if v < 8 else sums[8:16, :]
        turned = 16 * v % 128
        flat[v * 8 : v * 8 + 8, :] = pltpu.roll(source, 128 - turned, 1) if turned else source
    for j in range(SIZE):
        square[j, j:SIZE, :] = flat[OFFSET[j] : OFFSET[j] + SIZE - j, 0:NODES]
        for i in range(j):
            place = OFFSET[i] + j - i
            square[j, i : i + 1, :] = flat[place : place + 1, 0:NODES]
    row = lax.broadcasted_iota(jnp.int32, (SIZE, NODES), 0)
    columns = []
    for j in range(SIZE):
        added = jnp.where(row == j, shift[j : j + 1, :], 0.0)
        columns.append(square[j] + added)
    for j in range(SIZE):
        current = columns[j]
        here = row == j
        scale = 1.0 / current[j : j + 1, :]
        scaled = jnp.where(here, -scale, current * scale)
        for k in range(SIZE):
            if k == j:
                continue
            kept = jnp.where(here, 0.0, columns[k])
            columns[k] = kept - scaled * current[k : k + 1, :]
        columns[j] = scaled
    for j in range(SIZE):
        out[j] = -columns[j]


def shards(factors, dest_device, dest_node, live_count, shift):
    vmem = pl.BlockSpec(memory_space=pltpu.VMEM)
    in_hbm = functools.partial(pltpu.with_memory_space_constraint, memory_space=pltpu.HBM)
    sums = pl.pallas_call(
        exchange_kernel,
        out_shape=jax.ShapeDtypeStruct((16, 128), F32),
        in_specs=[pl.BlockSpec(memory_space=pltpu.HBM)] * 3
        + [pl.BlockSpec(memory_space=pltpu.SMEM)],
        out_specs=vmem,
        scratch_shapes=[
            pltpu.VMEM((SIZE, SIZE, COUNT), BF16),
            pltpu.VMEM((1, COUNT), jnp.int32),
            pltpu.VMEM((1, COUNT), jnp.int32),
            pltpu.SemaphoreType.DMA((3,)),
            pltpu.VMEM((208, COUNT), BF16),
            pltpu.VMEM((3, 208, 128), F32),
            pltpu.VMEM((3, ROWS, 128), F32),
            pltpu.VMEM((8, MESSAGE, 128), F32),
            pltpu.VMEM((8, MESSAGE, 128), F32),
            pltpu.VMEM((8, ROWS, 128), F32),
            pltpu.VMEM((8, ROWS, 128), F32),
            pltpu.VMEM((8, 16, 128), F32),
            pltpu.VMEM((8, 16, 128), F32),
        ]
        + [pltpu.SemaphoreType.DMA((8,))] * 6,
        compiler_params=pltpu.CompilerParams(
            collective_id=0, has_side_effects=True, vmem_limit_bytes=16 << 20
        ),
    )(
        in_hbm(factors),
        in_hbm(dest_device.reshape(1, COUNT)),
        in_hbm(dest_node.reshape(1, COUNT)),
        live_count,
    )
    return pl.pallas_call(
        inverse_kernel,
        out_shape=jax.ShapeDtypeStruct((SIZE, SIZE, NODES), F32),
        in_specs=[vmem, vmem],
        out_specs=vmem,
        scratch_shapes=[pltpu.VMEM((ROWS, 128), F32), pltpu.VMEM((SIZE, SIZE, NODES), F32)],
        compiler_params=pltpu.CompilerParams(vmem_limit_bytes=4 << 20),
    )(sums, shift)


def solution(mesh):
    placed = (
        P(None, None, ("elem", "node")),
        P(("elem", "node"), None),
        P(("elem", "node"), None),
        P(("elem", "node")),
        P(None, ("elem", "node")),
    )
    return jax.shard_map(
        shards,
        mesh=mesh,
        in_specs=placed,
        out_specs=P(None, None, ("elem", "node")),
        check_vma=False,
    )
```

```python
import functools

import jax
import jax.numpy as jnp
from jax import lax
from jax.experimental import pallas as pl
from jax.experimental.pallas import tpu as pltpu
from jax.sharding import PartitionSpec as P

MESH = pl.DeviceIdType.MESH
F32 = jnp.float32
BF16 = jnp.bfloat16
SIZE = 12
COUNT = 1024
NODES = 16
NX, NY, NZ, NC = 4, 8, 8, 2
OFFSET = [a * SIZE - a * (a - 1) // 2 for a in range(SIZE)]
ROWS = 80
MESSAGE = 120


def lanes(shape):
    return lax.broadcasted_iota(jnp.int32, shape, len(shape) - 1)


def ranks_of(owner):
    counts = [jnp.zeros((8, 128), F32) for _ in range(8)]
    rows = [owner[:, b * 128 : (b + 1) * 128] for b in range(8)]
    before = lax.broadcasted_iota(jnp.int32, (128, 128), 0) < lanes((128, 128))
    for b in range(8):
        column = jnp.broadcast_to(rows[b], (128, 128)).T
        for later in range(b, 8):
            same = column == rows[later]
            if later == b:
                same = same & before
            hits = jnp.where(same, 1.0, 0.0)
            counts[later] = counts[later] + jnp.sum(hits.reshape(16, 8, 128), axis=0)
    return jnp.concatenate([jnp.sum(c, axis=0, keepdims=True) for c in counts], axis=1)


def exchange_kernel(
    factors_in,
    owner_in,
    node_in,
    live_ref,
    out,
    factors,
    owner_ref,
    node_ref,
    isem,
    lhs,
    routed,
    packed,
    send1,
    recv1,
    dense,
    recv2,
    send3,
    recv3,
    ssem1,
    rsem1,
    ssem2,
    rsem2,
    ssem3,
    rsem3,
):
    inputs = [
        pltpu.make_async_copy(source, target, isem.at[n])
        for n, (source, target) in enumerate(
            [(owner_in, owner_ref), (node_in, node_ref), (factors_in, factors)]
        )
    ]
    for copy in inputs:
        copy.start()
    elem = lax.axis_index("elem")
    z = lax.axis_index("node")
    core = lax.rem(elem, NC)
    x = lax.rem(elem // NC, NX)
    y = elem // (NC * NX)

    def device(y_at, x_at, core_at, z_at):
        return ((y_at * NX + x_at) * NC + core_at, z_at)

    def partner1(i):
        return device(y, lax.rem(x + i // 2, NX), lax.rem(core + i, NC), z)

    def partner2(i):
        return device(lax.rem(y + i * (1 - core), NY), x, core, lax.rem(z + i * core, NZ))

    def partner3(i):
        return device(lax.rem(y + i * core, NY), x, core, lax.rem(z + i * (1 - core), NZ))

    barrier = pltpu.get_barrier_semaphore()
    for partner in (partner1, partner2, partner3):
        for i in range(1, 8):
            pl.semaphore_signal(barrier, inc=1, device_id=partner(i), device_id_type=MESH)

    first = y * (1 - core) + z * core
    second = z * (1 - core) + y * core

    inputs[0].wait()
    owner = owner_ref[...]
    rank = ranks_of(owner.astype(F32)).astype(jnp.int32)
    owner_z = owner & 7
    owner_core = (owner >> 3) & 1
    owner_x = (owner >> 4) & 3
    owner_y = owner >> 6
    other = owner_core ^ core
    step = (owner_x - x + NX) & 3
    slot = jnp.where(rank < 2, other * 128 + rank * 64, 256 + other * 64)
    outer = owner_y * (1 - owner_core) + owner_z * owner_core
    inner = owner_z * (1 - owner_core) + owner_y * owner_core
    lane = (outer * 8 + inner + ((2 * step + other) & 3) * 16) & 63
    slot = slot + step * 384 + lane
    slot = jnp.where(lanes((1, COUNT)) < live_ref[0], slot, -1)

    inputs[1].wait()
    inputs[2].wait()
    for a in range(SIZE):
        lhs[a * 16 : a * 16 + SIZE, :] = factors[a]
    lhs[192:208, :] = jnp.broadcast_to(node_ref[...].astype(F32), (16, COUNT)).astype(BF16)

    low = lanes((40, 128)) < 64

    def route(step, slot_at):
        wanted = lax.broadcasted_iota(jnp.int32, (384, COUNT), 0)
        choice = jnp.where(wanted == slot - step * 384, 1.0, 0.0).astype(BF16)
        result = lax.dot_general(
            lhs[...], choice, (((1,), (1,)), ((), ())), preferred_element_type=F32
        )
        for t in range(3):
            routed[slot_at * 3 + t] = result[:, t * 128 : (t + 1) * 128]

    def multiply(slot_at):
        for t in range(3):
            source = slot_at * 3 + t
            total = [None] * SIZE
            for k in range(SIZE):
                column = routed[source, pl.ds(k, SIZE, stride=16), :]
                for a in range(SIZE):
                    term = routed[source, a * 16 + k : a * 16 + k + 1, :] * column
                    total[a] = term if k == 0 else total[a] + term
            for a in range(SIZE):
                packed[source, OFFSET[a] : OFFSET[a] + SIZE - a, :] = total[a][a:SIZE]
            packed[source, 78:80, :] = routed[source, 192:194, :]
        upper, bottom = packed[slot_at * 3 + 2, 0:40, :], packed[slot_at * 3 + 2, 40:80, :]
        first_half = jnp.where(low, upper, pltpu.roll(bottom, 64, 1))
        second_half = jnp.where(low, pltpu.roll(upper, 64, 1), bottom)
        return first_half, second_half

    def fill(target, index, part, half):
        target[index, 0:ROWS, :] = packed[part]
        target[index, ROWS:MESSAGE, :] = half

    def copy1(i):
        return pltpu.make_async_remote_copy(
            src_ref=send1.at[i],
            dst_ref=recv1.at[i],
            send_sem=ssem1.at[i],
            recv_sem=rsem1.at[i],
            device_id=partner1(i),
            device_id_type=MESH,
        )

    def pair(step, slot_at):
        first_half, second_half = multiply(slot_at)
        fill(recv1 if step == 0 else send1, 2 * step, slot_at * 3, first_half)
        fill(send1, 2 * step + 1, slot_at * 3 + 1, second_half)

    def start(step):
        if step:
            copy1(2 * step).start()
        copy1(2 * step + 1).start()

    route(1, 0)
    pair(1, 0)
    route(3, 1)
    pl.semaphore_wait(barrier, 21)
    start(1)
    pair(3, 1)
    route(2, 0)
    start(3)
    pair(2, 0)
    route(0, 1)
    start(2)
    pair(0, 1)
    start(0)

    base = (lanes((1, 256)) & 15) * 16
    block = (lanes((1, 256)) & 63) >> 4
    low_row = lanes((1, 128)) < 64
    wanted = lax.broadcasted_iota(jnp.int32, (256, 256), 0)

    def batch(begin, finish):
        for delta in (2, 1, 3, 0):
            part = lax.rem(first // 2 + delta, 4)
            values = ids = None
            for source in range(4):
                i = begin + source
                half = recv1[i, ROWS:MESSAGE, :]
                spread = jnp.concatenate(
                    [jnp.where(low, half, 0.0), jnp.where(low, 0.0, half)], axis=0
                )
                value = jnp.concatenate([recv1[i, 0:ROWS, :], spread], axis=1)
                ids_half = recv1[i, ROWS + 38 : ROWS + 39, :]
                ids_half = jnp.where(low_row, pltpu.roll(ids_half, 64, 1), ids_half)
                ident = jnp.concatenate([recv1[i, 78:79, :], ids_half], axis=1)
                here = block == lax.rem(part + source, 4)
                values = value if source == 0 else jnp.where(here, value, values)
                ids = ident if source == 0 else jnp.where(here, ident, ids)
            place = base + ids.astype(jnp.int32)
            high = values.astype(BF16)
            rest = values - high.astype(F32)
            middle = rest.astype(BF16)
            tail = (rest - middle.astype(F32)).astype(BF16)
            pieces = jnp.concatenate([high, middle, tail], axis=0)
            choice = jnp.where(wanted == place, 1.0, 0.0).astype(BF16)
            found = lax.dot_general(
                pieces, choice, (((1,), (1,)), ((), ())), preferred_element_type=F32
            )
            found = found[0:ROWS] + found[ROWS : 2 * ROWS] + found[2 * ROWS : 3 * ROWS]
            for side in range(2):
                piece = found[:, side * 128 : side * 128 + 128]
                if begin:
                    piece = dense[2 * part + side] + piece
                dense[2 * part + side] = piece
            finish(delta)

    def copy2(target, source):
        return pltpu.make_async_remote_copy(
            src_ref=dense.at[target],
            dst_ref=recv2.at[source],
            send_sem=ssem2.at[target],
            recv_sem=rsem2.at[source],
            device_id=device(
                target * (1 - core) + y * core, x, core, z * (1 - core) + target * core
            ),
            device_id_type=MESH,
        )

    def ship(delta):
        part = lax.rem(first // 2 + delta, 4)
        copy2(2 * part, first).start()
        copy2(2 * part + 1, first).start()

    def after(delta):
        if delta == 1:
            ship(2)
        elif delta == 3:
            ship(1)
        elif delta == 0:
            ship(3)
            copy2(first + 1 - 2 * lax.rem(first, 2), first).start()

    for i in (1, 2, 3):
        copy1(i).wait_recv()
    batch(0, lambda delta: None)
    for i in (6, 7, 4, 5):
        copy1(i).wait_recv()
    batch(4, after)

    total = dense[first]
    for i in (1, 7, 2, 6, 3, 5, 4):
        source = lax.rem(first + i, 8)
        copy2(source, source).wait_recv()
        total = total + recv2[source]

    lane_full = lanes((8, 128))

    def swap(tiles):
        for span in (4, 2, 1):
            width = span * 16
            lower = (lane_full & width) == 0
            result = list(tiles)
            for v in range(8):
                if v & span:
                    continue
                one, two = tiles[v], tiles[v + span]
                result[v] = jnp.where(lower, one, pltpu.roll(two, width, 1))
                result[v + span] = jnp.where(lower, pltpu.roll(one, 128 - width, 1), two)
            tiles = result
        return tiles

    rows = [total[v * 8 : v * 8 + 8] for v in range(10)]
    empty = jnp.zeros((8, 128), F32)
    main = swap(rows[0:8])
    extra = swap(rows[8:10] + [empty] * 6)
    for q in range(8):
        send3[q, 0:8, :] = main[q]
        send3[q, 8:16, :] = extra[q]

    def copy3(i):
        return pltpu.make_async_remote_copy(
            src_ref=send3.at[lax.rem(second + i, 8)],
            dst_ref=recv3.at[i],
            send_sem=ssem3.at[i],
            recv_sem=rsem3.at[i],
            device_id=partner3(i),
            device_id_type=MESH,
        )

    for i in (4, 3, 5, 2, 6, 1, 7):
        copy3(i).start()
    result = send3[second]
    for i in (1, 7, 2, 6, 3, 5, 4):
        copy3(i).wait_recv()
        result = result + recv3[i]
    out[...] = result
    for i in range(1, 8):
        copy1(i).wait_send()
        copy2(lax.rem(first + i, 8), first).wait_send()
        copy3(i).wait_send()


def inverse_kernel(sums, shift, out, flat, square):
    for v in range(10):
        source = sums[0:8, :] if v < 8 else sums[8:16, :]
        turned = 16 * v % 128
        flat[v * 8 : v * 8 + 8, :] = pltpu.roll(source, 128 - turned, 1) if turned else source
    for j in range(SIZE):
        square[j, j:SIZE, :] = flat[OFFSET[j] : OFFSET[j] + SIZE - j, 0:NODES]
        for i in range(j):
            place = OFFSET[i] + j - i
            square[j, i : i + 1, :] = flat[place : place + 1, 0:NODES]
    row = lax.broadcasted_iota(jnp.int32, (SIZE, NODES), 0)
    columns = []
    for j in range(SIZE):
        added = jnp.where(row == j, shift[j : j + 1, :], 0.0)
        columns.append(square[j] + added)
    for j in range(SIZE):
        current = columns[j]
        here = row == j
        scale = 1.0 / current[j : j + 1, :]
        scaled = jnp.where(here, -scale, current * scale)
        for k in range(SIZE):
            if k == j:
                continue
            kept = jnp.where(here, 0.0, columns[k])
            columns[k] = kept - scaled * current[k : k + 1, :]
        columns[j] = scaled
    for j in range(SIZE):
        out[j] = -columns[j]


def shards(factors, dest_device, dest_node, live_count, shift):
    vmem = pl.BlockSpec(memory_space=pltpu.VMEM)
    in_hbm = functools.partial(pltpu.with_memory_space_constraint, memory_space=pltpu.HBM)
    sums = pl.pallas_call(
        exchange_kernel,
        out_shape=jax.ShapeDtypeStruct((16, 128), F32),
        in_specs=[pl.BlockSpec(memory_space=pltpu.HBM)] * 3
        + [pl.BlockSpec(memory_space=pltpu.SMEM)],
        out_specs=vmem,
        scratch_shapes=[
            pltpu.VMEM((SIZE, SIZE, COUNT), BF16),
            pltpu.VMEM((1, COUNT), jnp.int32),
            pltpu.VMEM((1, COUNT), jnp.int32),
            pltpu.SemaphoreType.DMA((3,)),
            pltpu.VMEM((208, COUNT), BF16),
            pltpu.VMEM((6, 208, 128), F32),
            pltpu.VMEM((6, ROWS, 128), F32),
            pltpu.VMEM((8, MESSAGE, 128), F32),
            pltpu.VMEM((8, MESSAGE, 128), F32),
            pltpu.VMEM((8, ROWS, 128), F32),
            pltpu.VMEM((8, ROWS, 128), F32),
            pltpu.VMEM((8, 16, 128), F32),
            pltpu.VMEM((8, 16, 128), F32),
        ]
        + [pltpu.SemaphoreType.DMA((8,))] * 6,
        compiler_params=pltpu.CompilerParams(
            collective_id=0, has_side_effects=True, vmem_limit_bytes=16 << 20
        ),
    )(
        in_hbm(factors),
        in_hbm(dest_device.reshape(1, COUNT)),
        in_hbm(dest_node.reshape(1, COUNT)),
        live_count,
    )
    return pl.pallas_call(
        inverse_kernel,
        out_shape=jax.ShapeDtypeStruct((SIZE, SIZE, NODES), F32),
        in_specs=[vmem, vmem],
        out_specs=vmem,
        scratch_shapes=[pltpu.VMEM((ROWS, 128), F32), pltpu.VMEM((SIZE, SIZE, NODES), F32)],
        compiler_params=pltpu.CompilerParams(vmem_limit_bytes=4 << 20),
    )(sums, shift)


def solution(mesh):
    placed = (
        P(None, None, ("elem", "node")),
        P(("elem", "node"), None),
        P(("elem", "node"), None),
        P(("elem", "node")),
        P(None, ("elem", "node")),
    )
    return jax.shard_map(
        shards,
        mesh=mesh,
        in_specs=placed,
        out_specs=P(None, None, ("elem", "node")),
        check_vma=False,
    )
```

```python
import functools

import jax
import jax.numpy as jnp
from jax import lax
from jax.experimental import pallas as pl
from jax.experimental.pallas import tpu as pltpu
from jax.sharding import PartitionSpec as P

MESH = pl.DeviceIdType.MESH
F32 = jnp.float32
BF16 = jnp.bfloat16
SIZE = 12
COUNT = 1024
NODES = 16
NX, NY, NZ, NC = 4, 8, 8, 2
OFFSET = [a * SIZE - a * (a - 1) // 2 for a in range(SIZE)]
ROWS = 80
MESSAGE = 120


def lanes(shape):
    return lax.broadcasted_iota(jnp.int32, shape, len(shape) - 1)


def ranks_of(owner):
    counts = [jnp.zeros((8, 128), F32) for _ in range(8)]
    rows = [owner[:, b * 128 : (b + 1) * 128] for b in range(8)]
    before = lax.broadcasted_iota(jnp.int32, (128, 128), 0) < lanes((128, 128))
    for b in range(8):
        column = jnp.broadcast_to(rows[b], (128, 128)).T
        for later in range(b, 8):
            same = column == rows[later]
            if later == b:
                same = same & before
            hits = jnp.where(same, 1.0, 0.0)
            counts[later] = counts[later] + jnp.sum(hits.reshape(16, 8, 128), axis=0)
    return jnp.concatenate([jnp.sum(c, axis=0, keepdims=True) for c in counts], axis=1)


def wait_for(buffer, begin, count, semaphore):
    span = buffer.at[pl.ds(begin, count)]
    pltpu.make_async_copy(span, span, semaphore).wait()


def exchange_kernel(
    factors_in,
    owner_in,
    node_in,
    live_ref,
    out,
    factors,
    owner_ref,
    node_ref,
    isem,
    lhs,
    routed,
    packed,
    send1,
    recv1,
    dense,
    recv2,
    send3,
    recv3,
    sent,
    arrived,
    ready,
    all_ready,
):
    inputs = [
        pltpu.make_async_copy(source, target, isem.at[n])
        for n, (source, target) in enumerate(
            [(owner_in, owner_ref), (node_in, node_ref), (factors_in, factors)]
        )
    ]
    for copy in inputs:
        copy.start()
    elem = lax.axis_index("elem")
    z = lax.axis_index("node")
    core = lax.rem(elem, NC)
    x = lax.rem(elem // NC, NX)
    y = elem // (NC * NX)

    def device(y_at, x_at, core_at, z_at):
        return ((y_at * NX + x_at) * NC + core_at, z_at)

    def partner1(i):
        return device(y, lax.rem(x + i // 2, NX), lax.rem(core + i, NC), z)

    def partner2(i):
        return device(lax.rem(y + i * (1 - core), NY), x, core, lax.rem(z + i * core, NZ))

    def partner3(i):
        return device(lax.rem(y + i * core, NY), x, core, lax.rem(z + i * (1 - core), NZ))

    barrier = pltpu.get_barrier_semaphore()
    near = [partner(i) for partner in (partner2, partner3) for i in (1, 7)]
    next_near = [partner(i) for partner in (partner2, partner3) for i in (2, 6)]
    for target in near + [partner1(i) for i in range(1, 8)]:
        pl.semaphore_signal(barrier, inc=1, device_id=target, device_id_type=MESH)

    first = y * (1 - core) + z * core
    second = z * (1 - core) + y * core

    inputs[0].wait()
    owner = owner_ref[...]
    rank = ranks_of(owner.astype(F32)).astype(jnp.int32)
    owner_z = owner & 7
    owner_core = (owner >> 3) & 1
    owner_x = (owner >> 4) & 3
    owner_y = owner >> 6
    other = owner_core ^ core
    step = (owner_x - x + NX) & 3
    slot = jnp.where(rank < 2, other * 128 + rank * 64, 256 + other * 64)
    outer = owner_y * (1 - owner_core) + owner_z * owner_core
    inner = owner_z * (1 - owner_core) + owner_y * owner_core
    lane = (outer * 8 + inner + ((2 * step + other) & 3) * 16) & 63
    slot = slot + step * 384 + lane
    slot = jnp.where(lanes((1, COUNT)) < live_ref[0], slot, -1)

    inputs[1].wait()
    inputs[2].wait()
    for a in range(SIZE):
        lhs[a * 16 : a * 16 + SIZE, :] = factors[a]
    lhs[192:208, :] = jnp.broadcast_to(node_ref[...].astype(F32), (16, COUNT)).astype(BF16)

    low = lanes((40, 128)) < 64

    def route(step, slot_at):
        wanted = lax.broadcasted_iota(jnp.int32, (384, COUNT), 0)
        choice = jnp.where(wanted == slot - step * 384, 1.0, 0.0).astype(BF16)
        result = lax.dot_general(
            lhs[...], choice, (((1,), (1,)), ((), ())), preferred_element_type=F32
        )
        for t in range(3):
            routed[slot_at * 3 + t] = result[:, t * 128 : (t + 1) * 128]

    def multiply(slot_at):
        for t in range(3):
            source = slot_at * 3 + t
            total = [None] * SIZE
            for k in range(SIZE):
                column = routed[source, pl.ds(k, SIZE, stride=16), :]
                for a in range(SIZE):
                    term = routed[source, a * 16 + k : a * 16 + k + 1, :] * column
                    total[a] = term if k == 0 else total[a] + term
            for a in range(SIZE):
                packed[source, OFFSET[a] : OFFSET[a] + SIZE - a, :] = total[a][a:SIZE]
            packed[source, 78:80, :] = routed[source, 192:194, :]
        upper, bottom = packed[slot_at * 3 + 2, 0:40, :], packed[slot_at * 3 + 2, 40:80, :]
        first_half = jnp.where(low, upper, pltpu.roll(bottom, 64, 1))
        second_half = jnp.where(low, pltpu.roll(upper, 64, 1), bottom)
        return first_half, second_half

    def fill(target, index, part, half):
        target[index, 0:ROWS, :] = packed[part]
        target[index, ROWS:MESSAGE, :] = half

    def copy1(i):
        return pltpu.make_async_remote_copy(
            src_ref=send1.at[i],
            dst_ref=recv1.at[i],
            send_sem=sent.at[0],
            recv_sem=arrived.at[i // 4],
            device_id=partner1(i),
            device_id_type=MESH,
        )

    def pair(step, slot_at):
        first_half, second_half = multiply(slot_at)
        fill(recv1 if step == 0 else send1, 2 * step, slot_at * 3, first_half)
        fill(send1, 2 * step + 1, slot_at * 3 + 1, second_half)

    def start(step):
        if step:
            copy1(2 * step).start()
        copy1(2 * step + 1).start()

    route(1, 0)
    pair(1, 0)
    route(3, 1)
    pl.semaphore_wait(barrier, 11)
    start(1)
    for target in near:
        pl.semaphore_signal(ready, inc=1, device_id=target, device_id_type=MESH)
    pair(3, 1)
    route(2, 0)
    start(3)
    pair(2, 0)
    route(0, 1)
    start(2)
    pair(0, 1)
    start(0)
    pl.semaphore_wait(ready, 4)
    for target in next_near:
        pl.semaphore_signal(all_ready, inc=1, device_id=target, device_id_type=MESH)

    base = (lanes((1, 256)) & 15) * 16
    block = (lanes((1, 256)) & 63) >> 4
    low_row = lanes((1, 128)) < 64
    wanted = lax.broadcasted_iota(jnp.int32, (256, 256), 0)

    def batch(begin, finish):
        for delta in (2, 1, 3, 0):
            part = lax.rem(first // 2 + delta, 4)
            values = ids = None
            for source in range(4):
                i = begin + source
                half = recv1[i, ROWS:MESSAGE, :]
                spread = jnp.concatenate(
                    [jnp.where(low, half, 0.0), jnp.where(low, 0.0, half)], axis=0
                )
                value = jnp.concatenate([recv1[i, 0:ROWS, :], spread], axis=1)
                ids_half = recv1[i, ROWS + 38 : ROWS + 39, :]
                ids_half = jnp.where(low_row, pltpu.roll(ids_half, 64, 1), ids_half)
                ident = jnp.concatenate([recv1[i, 78:79, :], ids_half], axis=1)
                here = block == lax.rem(part + source, 4)
                values = value if source == 0 else jnp.where(here, value, values)
                ids = ident if source == 0 else jnp.where(here, ident, ids)
            place = base + ids.astype(jnp.int32)
            high = values.astype(BF16)
            rest = values - high.astype(F32)
            middle = rest.astype(BF16)
            tail = (rest - middle.astype(F32)).astype(BF16)
            pieces = jnp.concatenate([high, middle, tail], axis=0)
            choice = jnp.where(wanted == place, 1.0, 0.0).astype(BF16)
            found = lax.dot_general(
                pieces, choice, (((1,), (1,)), ((), ())), preferred_element_type=F32
            )
            found = found[0:ROWS] + found[ROWS : 2 * ROWS] + found[2 * ROWS : 3 * ROWS]
            for side in range(2):
                piece = found[:, side * 128 : side * 128 + 128]
                if begin:
                    piece = dense[2 * part + side] + piece
                dense[2 * part + side] = piece
            finish(delta)

    def copy2(target, source):
        return pltpu.make_async_remote_copy(
            src_ref=dense.at[target],
            dst_ref=recv2.at[source],
            send_sem=sent.at[1],
            recv_sem=arrived.at[2],
            device_id=device(
                target * (1 - core) + y * core, x, core, z * (1 - core) + target * core
            ),
            device_id_type=MESH,
        )

    def ship(delta):
        part = lax.rem(first // 2 + delta, 4)
        copy2(2 * part, first).start()
        copy2(2 * part + 1, first).start()

    def after(delta):
        if delta:
            ship(delta)
        else:
            copy2(first + 1 - 2 * lax.rem(first, 2), first).start()

    wait_for(recv1, 1, 3, arrived.at[0])
    batch(0, lambda delta: None)
    wait_for(recv1, 4, 4, arrived.at[1])
    pl.semaphore_wait(all_ready, 4)
    batch(4, after)

    total = dense[first]
    wait_for(recv2, 0, 7, arrived.at[2])
    for i in range(1, 8):
        total = total + recv2[lax.rem(first + i, 8)]

    lane_full = lanes((8, 128))

    def swap(tiles):
        for span in (4, 2, 1):
            width = span * 16
            lower = (lane_full & width) == 0
            result = list(tiles)
            for v in range(8):
                if v & span:
                    continue
                one, two = tiles[v], tiles[v + span]
                result[v] = jnp.where(lower, one, pltpu.roll(two, width, 1))
                result[v + span] = jnp.where(lower, pltpu.roll(one, 128 - width, 1), two)
            tiles = result
        return tiles

    rows = [total[v * 8 : v * 8 + 8] for v in range(10)]
    empty = jnp.zeros((8, 128), F32)
    main = swap(rows[0:8])
    extra = swap(rows[8:10] + [empty] * 6)
    for q in range(8):
        send3[q, 0:8, :] = main[q]
        send3[q, 8:16, :] = extra[q]

    def copy3(i):
        return pltpu.make_async_remote_copy(
            src_ref=send3.at[lax.rem(second + i, 8)],
            dst_ref=recv3.at[i],
            send_sem=sent.at[2],
            recv_sem=arrived.at[3],
            device_id=partner3(i),
            device_id_type=MESH,
        )

    for i in (4, 3, 5, 2, 6, 1, 7):
        copy3(i).start()
    result = send3[second]
    wait_for(recv3, 1, 7, arrived.at[3])
    for i in range(1, 8):
        result = result + recv3[i]
    out[...] = result
    wait_for(recv1, 1, 7, sent.at[0])
    wait_for(recv2, 0, 7, sent.at[1])
    wait_for(recv3, 1, 7, sent.at[2])


def inverse_kernel(sums, shift, out, flat, square):
    for v in range(10):
        source = sums[0:8, :] if v < 8 else sums[8:16, :]
        turned = 16 * v % 128
        flat[v * 8 : v * 8 + 8, :] = pltpu.roll(source, 128 - turned, 1) if turned else source
    for j in range(SIZE):
        square[j, j:SIZE, :] = flat[OFFSET[j] : OFFSET[j] + SIZE - j, 0:NODES]
        for i in range(j):
            place = OFFSET[i] + j - i
            square[j, i : i + 1, :] = flat[place : place + 1, 0:NODES]
    row = lax.broadcasted_iota(jnp.int32, (SIZE, NODES), 0)
    columns = []
    for j in range(SIZE):
        added = jnp.where(row == j, shift[j : j + 1, :], 0.0)
        columns.append(square[j] + added)
    for j in range(SIZE):
        current = columns[j]
        here = row == j
        scale = 1.0 / current[j : j + 1, :]
        scaled = jnp.where(here, -scale, current * scale)
        for k in range(SIZE):
            if k == j:
                continue
            kept = jnp.where(here, 0.0, columns[k])
            columns[k] = kept - scaled * current[k : k + 1, :]
        columns[j] = scaled
    for j in range(SIZE):
        out[j] = -columns[j]


def shards(factors, dest_device, dest_node, live_count, shift):
    vmem = pl.BlockSpec(memory_space=pltpu.VMEM)
    in_hbm = functools.partial(pltpu.with_memory_space_constraint, memory_space=pltpu.HBM)
    sums = pl.pallas_call(
        exchange_kernel,
        out_shape=jax.ShapeDtypeStruct((16, 128), F32),
        in_specs=[pl.BlockSpec(memory_space=pltpu.HBM)] * 3
        + [pl.BlockSpec(memory_space=pltpu.SMEM)],
        out_specs=vmem,
        scratch_shapes=[
            pltpu.VMEM((SIZE, SIZE, COUNT), BF16),
            pltpu.VMEM((1, COUNT), jnp.int32),
            pltpu.VMEM((1, COUNT), jnp.int32),
            pltpu.SemaphoreType.DMA((3,)),
            pltpu.VMEM((208, COUNT), BF16),
            pltpu.VMEM((6, 208, 128), F32),
            pltpu.VMEM((6, ROWS, 128), F32),
            pltpu.VMEM((8, MESSAGE, 128), F32),
            pltpu.VMEM((8, MESSAGE, 128), F32),
            pltpu.VMEM((8, ROWS, 128), F32),
            pltpu.VMEM((8, ROWS, 128), F32),
            pltpu.VMEM((8, 16, 128), F32),
            pltpu.VMEM((8, 16, 128), F32),
        ]
        + [pltpu.SemaphoreType.DMA((3,)), pltpu.SemaphoreType.DMA((4,))]
        + [pltpu.SemaphoreType.REGULAR] * 2,
        compiler_params=pltpu.CompilerParams(
            collective_id=0, has_side_effects=True, vmem_limit_bytes=16 << 20
        ),
    )(
        in_hbm(factors),
        in_hbm(dest_device.reshape(1, COUNT)),
        in_hbm(dest_node.reshape(1, COUNT)),
        live_count,
    )
    return pl.pallas_call(
        inverse_kernel,
        out_shape=jax.ShapeDtypeStruct((SIZE, SIZE, NODES), F32),
        in_specs=[vmem, vmem],
        out_specs=vmem,
        scratch_shapes=[pltpu.VMEM((ROWS, 128), F32), pltpu.VMEM((SIZE, SIZE, NODES), F32)],
        compiler_params=pltpu.CompilerParams(vmem_limit_bytes=4 << 20),
    )(sums, shift)


def solution(mesh):
    placed = (
        P(None, None, ("elem", "node")),
        P(("elem", "node"), None),
        P(("elem", "node"), None),
        P(("elem", "node")),
        P(None, ("elem", "node")),
    )
    return jax.shard_map(
        shards,
        mesh=mesh,
        in_specs=placed,
        out_specs=P(None, None, ("elem", "node")),
        check_vma=False,
    )
```

```python
import functools

import jax
import jax.numpy as jnp
from jax import lax
from jax.experimental import pallas as pl
from jax.experimental.pallas import tpu as pltpu
from jax.sharding import PartitionSpec as P

MESH = pl.DeviceIdType.MESH
F32 = jnp.float32
BF16 = jnp.bfloat16
SIZE = 12
COUNT = 1024
NODES = 16
NX, NY, NZ, NC = 4, 8, 8, 2
OFFSET = [1 + a * SIZE - a * (a - 1) // 2 for a in range(SIZE)]
ROWS = 80
MESSAGE = 120
CHUNKS = ((0, 48), (48, 32))


def lanes(shape):
    return lax.broadcasted_iota(jnp.int32, shape, len(shape) - 1)


def ranks_of(owner):
    counts = [jnp.zeros((8, 128), F32) for _ in range(8)]
    rows = [owner[:, b * 128 : (b + 1) * 128] for b in range(8)]
    before = lax.broadcasted_iota(jnp.int32, (128, 128), 0) < lanes((128, 128))
    for b in range(8):
        column = jnp.broadcast_to(rows[b], (128, 128)).T
        for later in range(b, 8):
            same = column == rows[later]
            if later == b:
                same = same & before
            hits = jnp.where(same, 1.0, 0.0)
            counts[later] = counts[later] + jnp.sum(hits.reshape(16, 8, 128), axis=0)
    return jnp.concatenate([jnp.sum(c, axis=0, keepdims=True) for c in counts], axis=1)


def wait_for(buffer, begin, count, semaphore, rows=None):
    span = buffer.at[pl.ds(begin, count)]
    if rows is not None:
        span = buffer.at[pl.ds(begin, count), pl.ds(*rows)]
    pltpu.make_async_copy(span, span, semaphore).wait()


def exchange_kernel(
    factors_in,
    owner_in,
    node_in,
    live_ref,
    out,
    factors,
    owner_ref,
    node_ref,
    isem,
    lhs,
    routed,
    packed,
    send1,
    recv1,
    dense,
    recv2,
    send3,
    recv3,
    sent,
    arrived,
    ready,
    all_ready,
):
    inputs = [
        pltpu.make_async_copy(source, target, isem.at[n])
        for n, (source, target) in enumerate(
            [(owner_in, owner_ref), (node_in, node_ref), (factors_in, factors)]
        )
    ]
    for copy in inputs:
        copy.start()
    elem = lax.axis_index("elem")
    z = lax.axis_index("node")
    core = lax.rem(elem, NC)
    x = lax.rem(elem // NC, NX)
    y = elem // (NC * NX)

    def device(y_at, x_at, core_at, z_at):
        return ((y_at * NX + x_at) * NC + core_at, z_at)

    def partner1(i):
        return device(y, lax.rem(x + i // 2, NX), lax.rem(core + i, NC), z)

    def partner2(i):
        return device(lax.rem(y + i * (1 - core), NY), x, core, lax.rem(z + i * core, NZ))

    def partner3(i):
        return device(lax.rem(y + i * core, NY), x, core, lax.rem(z + i * (1 - core), NZ))

    barrier = pltpu.get_barrier_semaphore()
    near = [partner(i) for partner in (partner2, partner3) for i in (1, 7)]
    next_near = [partner(i) for partner in (partner2, partner3) for i in (2, 6)]
    for target in near + [partner1(i) for i in range(1, 8)]:
        pl.semaphore_signal(barrier, inc=1, device_id=target, device_id_type=MESH)

    first = y * (1 - core) + z * core
    second = z * (1 - core) + y * core

    inputs[0].wait()
    owner = owner_ref[...]
    rank = ranks_of(owner.astype(F32)).astype(jnp.int32)
    owner_z = owner & 7
    owner_core = (owner >> 3) & 1
    owner_x = (owner >> 4) & 3
    owner_y = owner >> 6
    other = owner_core ^ core
    step = (owner_x - x + NX) & 3
    slot = jnp.where(rank < 2, other * 128 + rank * 64, 256 + other * 64)
    outer = owner_y * (1 - owner_core) + owner_z * owner_core
    inner = owner_z * (1 - owner_core) + owner_y * owner_core
    lane = (outer * 8 + inner + ((2 * step + other) & 3) * 16) & 63
    slot = slot + step * 384 + lane
    slot = jnp.where(lanes((1, COUNT)) < live_ref[0], slot, -1)

    inputs[1].wait()
    inputs[2].wait()
    for a in range(SIZE):
        lhs[a * 16 : a * 16 + SIZE, :] = factors[a]
    lhs[192:208, :] = jnp.broadcast_to(node_ref[...].astype(F32), (16, COUNT)).astype(BF16)

    def route(step, slot_at):
        wanted = lax.broadcasted_iota(jnp.int32, (384, COUNT), 0)
        choice = jnp.where(wanted == slot - step * 384, 1.0, 0.0).astype(BF16)
        result = lax.dot_general(
            lhs[...], choice, (((1,), (1,)), ((), ())), preferred_element_type=F32
        )
        for t in range(3):
            routed[slot_at * 3 + t] = result[:, t * 128 : (t + 1) * 128]

    def multiply(slot_at):
        for t in range(3):
            source = slot_at * 3 + t
            total = [None] * SIZE
            for k in range(SIZE):
                column = routed[source, pl.ds(k, SIZE, stride=16), :]
                for a in range(SIZE):
                    term = routed[source, a * 16 + k : a * 16 + k + 1, :] * column
                    total[a] = term if k == 0 else total[a] + term
            for a in range(SIZE):
                packed[source, OFFSET[a] : OFFSET[a] + SIZE - a, :] = total[a][a:SIZE]
            packed[source, 0:1, :] = routed[source, 192:193, :]
            packed[source, 79:80, :] = routed[source, 192:193, :]

    def fill(target, index, part, tail):
        for begin, rows in CHUNKS:
            place = begin * 3 // 2
            target[index, place : place + rows, :] = packed[part, begin : begin + rows, :]
            half = rows // 2
            upper = packed[tail, begin : begin + half, :]
            bottom = packed[tail, begin + half : begin + rows, :]
            low = lanes((half, 128)) < 64
            if part == tail - 2:
                both = jnp.where(low, upper, pltpu.roll(bottom, 64, 1))
            else:
                both = jnp.where(low, pltpu.roll(upper, 64, 1), bottom)
            target[index, place + rows : place + rows + half, :] = both

    def copy1(i, chunk):
        begin, rows = CHUNKS[chunk]
        span = pl.ds(begin * 3 // 2, rows * 3 // 2)
        return pltpu.make_async_remote_copy(
            src_ref=send1.at[i, span],
            dst_ref=recv1.at[i, span],
            send_sem=sent.at[0],
            recv_sem=arrived.at[chunk * 2 + i // 4],
            device_id=partner1(i),
            device_id_type=MESH,
        )

    def pair(step, slot_at):
        multiply(slot_at)
        fill(recv1 if step == 0 else send1, 2 * step, slot_at * 3, slot_at * 3 + 2)
        fill(send1, 2 * step + 1, slot_at * 3 + 1, slot_at * 3 + 2)

    def start(step, chunk):
        if step:
            copy1(2 * step, chunk).start()
        copy1(2 * step + 1, chunk).start()

    route(1, 0)
    pair(1, 0)
    route(3, 1)
    pl.semaphore_wait(barrier, 11)
    start(1, 0)
    for target in near:
        pl.semaphore_signal(ready, inc=1, device_id=target, device_id_type=MESH)
    pair(3, 1)
    route(2, 0)
    start(3, 0)
    pair(2, 0)
    route(0, 1)
    start(2, 0)
    pair(0, 1)
    start(0, 0)
    for step in (1, 3, 2, 0):
        start(step, 1)
    pl.semaphore_wait(ready, 4)
    for target in next_near:
        pl.semaphore_signal(all_ready, inc=1, device_id=target, device_id_type=MESH)

    base = (lanes((1, 256)) & 15) * 16
    block = (lanes((1, 256)) & 63) >> 4
    low_row = lanes((1, 128)) < 64
    wanted = lax.broadcasted_iota(jnp.int32, (256, 256), 0)

    def batch(begin, chunk):
        first_row, rows = CHUNKS[chunk]
        at = first_row * 3 // 2
        low = lanes((rows // 2, 128)) < 64
        for delta in (2, 1, 3, 0):
            part = lax.rem(first // 2 + delta, 4)
            values = ids = None
            for source in range(4):
                i = begin + source
                half = recv1[i, at + rows : at + rows * 3 // 2, :]
                spread = jnp.concatenate(
                    [jnp.where(low, half, 0.0), jnp.where(low, 0.0, half)], axis=0
                )
                value = jnp.concatenate([recv1[i, at : at + rows, :], spread], axis=1)
                ids_half = recv1[i, 48:49, :]
                ids_half = jnp.where(low_row, ids_half, pltpu.roll(ids_half, 64, 1))
                ident = jnp.concatenate([recv1[i, 0:1, :], ids_half], axis=1)
                here = block == lax.rem(part + source, 4)
                values = value if source == 0 else jnp.where(here, value, values)
                ids = ident if source == 0 else jnp.where(here, ident, ids)
            place = base + ids.astype(jnp.int32)
            high = values.astype(BF16)
            rest = values - high.astype(F32)
            middle = rest.astype(BF16)
            tail = (rest - middle.astype(F32)).astype(BF16)
            pieces = jnp.concatenate([high, middle, tail], axis=0)
            choice = jnp.where(wanted == place, 1.0, 0.0).astype(BF16)
            found = lax.dot_general(
                pieces, choice, (((1,), (1,)), ((), ())), preferred_element_type=F32
            )
            found = found[0:rows] + found[rows : 2 * rows] + found[2 * rows : 3 * rows]
            for side in range(2):
                piece = found[:, side * 128 : side * 128 + 128]
                if begin:
                    piece = dense[2 * part + side, first_row : first_row + rows, :] + piece
                dense[2 * part + side, first_row : first_row + rows, :] = piece
            if begin and delta:
                copy2(2 * part, first, chunk).start()
                copy2(2 * part + 1, first, chunk).start()
            elif begin:
                copy2(first + 1 - 2 * lax.rem(first, 2), first, chunk).start()

    def copy2(target, source, chunk):
        begin, rows = CHUNKS[chunk]
        return pltpu.make_async_remote_copy(
            src_ref=dense.at[target, pl.ds(begin, rows)],
            dst_ref=recv2.at[source, pl.ds(begin, rows)],
            send_sem=sent.at[1],
            recv_sem=arrived.at[4 + chunk],
            device_id=device(
                target * (1 - core) + y * core, x, core, z * (1 - core) + target * core
            ),
            device_id_type=MESH,
        )

    for chunk, (begin, rows) in enumerate(CHUNKS):
        part_rows = (begin * 3 // 2, rows * 3 // 2)
        wait_for(recv1, 1, 3, arrived.at[chunk * 2], part_rows)
        batch(0, chunk)
        wait_for(recv1, 4, 4, arrived.at[chunk * 2 + 1], part_rows)
        if chunk == 0:
            pl.semaphore_wait(all_ready, 4)
        batch(4, chunk)

    lane_full = lanes((8, 128))

    def swap(tiles):
        for span in (4, 2, 1):
            width = span * 16
            lower = (lane_full & width) == 0
            result = list(tiles)
            for v in range(8):
                if v & span:
                    continue
                one, two = tiles[v], tiles[v + span]
                result[v] = jnp.where(lower, one, pltpu.roll(two, width, 1))
                result[v + span] = jnp.where(lower, pltpu.roll(one, 128 - width, 1), two)
            tiles = result
        return tiles

    def copy3(i, chunk):
        return pltpu.make_async_remote_copy(
            src_ref=send3.at[lax.rem(second + i, 8), chunk],
            dst_ref=recv3.at[i, chunk],
            send_sem=sent.at[2],
            recv_sem=arrived.at[6],
            device_id=partner3(i),
            device_id_type=MESH,
        )

    empty = jnp.zeros((8, 128), F32)
    for chunk, (begin, rows) in enumerate(CHUNKS):
        wait_for(recv2, 0, 7, arrived.at[4 + chunk], (begin, rows))
        total = dense[first, begin : begin + rows, :]
        for i in range(1, 8):
            total = total + recv2[lax.rem(first + i, 8), begin : begin + rows, :]
        tiles = [total[v * 8 : v * 8 + 8] for v in range(rows // 8)]
        tiles = swap(tiles + [empty] * (8 - len(tiles)))
        for q in range(8):
            send3[q, chunk] = tiles[q]
        for i in (4, 3, 5, 2, 6, 1, 7):
            copy3(i, chunk).start()
    wait_for(recv3, 1, 7, arrived.at[6])
    for chunk in range(2):
        result = send3[second, chunk]
        for i in range(1, 8):
            result = result + recv3[i, chunk]
        out[chunk * 8 : chunk * 8 + 8, :] = result
    wait_for(recv1, 1, 7, sent.at[0])
    wait_for(recv2, 0, 7, sent.at[1])
    wait_for(recv3, 1, 7, sent.at[2])


def inverse_kernel(sums, shift, out, flat, square):
    for v in range(10):
        source = sums[0:8, :] if v < 6 else sums[8:16, :]
        turned = 16 * (v if v < 6 else v - 6)
        flat[v * 8 : v * 8 + 8, :] = pltpu.roll(source, 128 - turned, 1) if turned else source
    for j in range(SIZE):
        square[j, j:SIZE, :] = flat[OFFSET[j] : OFFSET[j] + SIZE - j, 0:NODES]
        for i in range(j):
            place = OFFSET[i] + j - i
            square[j, i : i + 1, :] = flat[place : place + 1, 0:NODES]
    row = lax.broadcasted_iota(jnp.int32, (SIZE, NODES), 0)
    columns = []
    for j in range(SIZE):
        added = jnp.where(row == j, shift[j : j + 1, :], 0.0)
        columns.append(square[j] + added)
    for j in range(SIZE):
        current = columns[j]
        here = row == j
        scale = 1.0 / current[j : j + 1, :]
        scaled = jnp.where(here, -scale, current * scale)
        for k in range(SIZE):
            if k == j:
                continue
            kept = jnp.where(here, 0.0, columns[k])
            columns[k] = kept - scaled * current[k : k + 1, :]
        columns[j] = scaled
    for j in range(SIZE):
        out[j] = -columns[j]


def shards(factors, dest_device, dest_node, live_count, shift):
    vmem = pl.BlockSpec(memory_space=pltpu.VMEM)
    in_hbm = functools.partial(pltpu.with_memory_space_constraint, memory_space=pltpu.HBM)
    sums = pl.pallas_call(
        exchange_kernel,
        out_shape=jax.ShapeDtypeStruct((16, 128), F32),
        in_specs=[pl.BlockSpec(memory_space=pltpu.HBM)] * 3
        + [pl.BlockSpec(memory_space=pltpu.SMEM)],
        out_specs=vmem,
        scratch_shapes=[
            pltpu.VMEM((SIZE, SIZE, COUNT), BF16),
            pltpu.VMEM((1, COUNT), jnp.int32),
            pltpu.VMEM((1, COUNT), jnp.int32),
            pltpu.SemaphoreType.DMA((3,)),
            pltpu.VMEM((208, COUNT), BF16),
            pltpu.VMEM((6, 208, 128), F32),
            pltpu.VMEM((6, ROWS, 128), F32),
            pltpu.VMEM((8, MESSAGE, 128), F32),
            pltpu.VMEM((8, MESSAGE, 128), F32),
            pltpu.VMEM((8, ROWS, 128), F32),
            pltpu.VMEM((8, ROWS, 128), F32),
            pltpu.VMEM((8, 2, 8, 128), F32),
            pltpu.VMEM((8, 2, 8, 128), F32),
        ]
        + [pltpu.SemaphoreType.DMA((3,)), pltpu.SemaphoreType.DMA((7,))]
        + [pltpu.SemaphoreType.REGULAR] * 2,
        compiler_params=pltpu.CompilerParams(
            collective_id=0, has_side_effects=True, vmem_limit_bytes=16 << 20
        ),
    )(
        in_hbm(factors),
        in_hbm(dest_device.reshape(1, COUNT)),
        in_hbm(dest_node.reshape(1, COUNT)),
        live_count,
    )
    return pl.pallas_call(
        inverse_kernel,
        out_shape=jax.ShapeDtypeStruct((SIZE, SIZE, NODES), F32),
        in_specs=[vmem, vmem],
        out_specs=vmem,
        scratch_shapes=[pltpu.VMEM((ROWS, 128), F32), pltpu.VMEM((SIZE, SIZE, NODES), F32)],
        compiler_params=pltpu.CompilerParams(vmem_limit_bytes=4 << 20),
    )(sums, shift)


def solution(mesh):
    placed = (
        P(None, None, ("elem", "node")),
        P(("elem", "node"), None),
        P(("elem", "node"), None),
        P(("elem", "node")),
        P(None, ("elem", "node")),
    )
    return jax.shard_map(
        shards,
        mesh=mesh,
        in_specs=placed,
        out_specs=P(None, None, ("elem", "node")),
        check_vma=False,
    )
```

```python
import functools

import jax
import jax.numpy as jnp
from jax import lax
from jax.experimental import pallas as pl
from jax.experimental.pallas import tpu as pltpu
from jax.sharding import PartitionSpec as P

MESH = pl.DeviceIdType.MESH
F32 = jnp.float32
BF16 = jnp.bfloat16
SIZE = 12
COUNT = 1024
NODES = 16
NX, NY, NZ, NC = 4, 8, 8, 2
OFFSET = [1 + a * SIZE - a * (a - 1) // 2 for a in range(SIZE)]
ROWS = 80
MESSAGE = 120
CHUNKS = ((0, 48), (48, 32))


def lanes(shape):
    return lax.broadcasted_iota(jnp.int32, shape, len(shape) - 1)


def ranks_of(owner):
    counts = [jnp.zeros((8, 128), F32) for _ in range(8)]
    rows = [owner[:, b * 128 : (b + 1) * 128] for b in range(8)]
    before = lax.broadcasted_iota(jnp.int32, (128, 128), 0) < lanes((128, 128))
    for b in range(8):
        column = jnp.broadcast_to(rows[b], (128, 128)).T
        for later in range(b, 8):
            same = column == rows[later]
            if later == b:
                same = same & before
            hits = jnp.where(same, 1.0, 0.0)
            counts[later] = counts[later] + jnp.sum(hits.reshape(16, 8, 128), axis=0)
    return jnp.concatenate([jnp.sum(c, axis=0, keepdims=True) for c in counts], axis=1)


def wait_for(buffer, begin, count, semaphore, rows=None):
    span = buffer.at[pl.ds(begin, count)]
    if rows is not None:
        span = buffer.at[pl.ds(begin, count), pl.ds(*rows)]
    pltpu.make_async_copy(span, span, semaphore).wait()


def exchange_kernel(
    factors_in,
    owner_in,
    node_in,
    live_ref,
    out,
    factors,
    owner_ref,
    node_ref,
    isem,
    lhs,
    routed,
    packed,
    send1,
    recv1,
    dense,
    recv2,
    send3,
    recv3,
    sent,
    arrived,
    ready,
    all_ready,
):
    inputs = [
        pltpu.make_async_copy(source, target, isem.at[n])
        for n, (source, target) in enumerate(
            [(owner_in, owner_ref), (node_in, node_ref), (factors_in, factors)]
        )
    ]
    for copy in inputs:
        copy.start()
    elem = lax.axis_index("elem")
    z = lax.axis_index("node")
    core = lax.rem(elem, NC)
    x = lax.rem(elem // NC, NX)
    y = elem // (NC * NX)

    def device(y_at, x_at, core_at, z_at):
        return ((y_at * NX + x_at) * NC + core_at, z_at)

    def partner1(i):
        return device(y, lax.rem(x + i // 2, NX), lax.rem(core + i, NC), z)

    def partner2(i):
        return device(lax.rem(y + i * core, NY), x, core, lax.rem(z + i * (1 - core), NZ))

    def partner3(i):
        return device(lax.rem(y + i * (1 - core), NY), x, core, lax.rem(z + i * core, NZ))

    barrier = pltpu.get_barrier_semaphore()
    near = [partner(i) for partner in (partner2, partner3) for i in (1, 7)]
    next_near = [partner(i) for partner in (partner2, partner3) for i in (2, 6)]
    for target in near + [partner1(i) for i in range(1, 8)]:
        pl.semaphore_signal(barrier, inc=1, device_id=target, device_id_type=MESH)

    first = y * core + z * (1 - core)
    second = z * core + y * (1 - core)

    inputs[0].wait()
    owner = owner_ref[...]
    rank = ranks_of(owner.astype(F32)).astype(jnp.int32)
    owner_z = owner & 7
    owner_core = (owner >> 3) & 1
    owner_x = (owner >> 4) & 3
    owner_y = owner >> 6
    other = owner_core ^ core
    step = (owner_x - x + NX) & 3
    slot = jnp.where(rank < 2, other * 128 + rank * 64, 256 + other * 64)
    outer = owner_y * owner_core + owner_z * (1 - owner_core)
    inner = owner_z * owner_core + owner_y * (1 - owner_core)
    lane = (outer * 8 + inner + ((2 * step + other) & 3) * 16) & 63
    slot = slot + step * 384 + lane
    slot = jnp.where(lanes((1, COUNT)) < live_ref[0], slot, -1)

    inputs[1].wait()
    inputs[2].wait()
    for a in range(SIZE):
        lhs[a * 16 : a * 16 + SIZE, :] = factors[a]
    lhs[192:208, :] = jnp.broadcast_to(node_ref[...].astype(F32), (16, COUNT)).astype(BF16)

    def route(step, slot_at):
        wanted = lax.broadcasted_iota(jnp.int32, (384, COUNT), 0)
        choice = jnp.where(wanted == slot - step * 384, 1.0, 0.0).astype(BF16)
        result = lax.dot_general(
            lhs[...], choice, (((1,), (1,)), ((), ())), preferred_element_type=F32
        )
        for t in range(3):
            routed[slot_at * 3 + t] = result[:, t * 128 : (t + 1) * 128]

    def multiply(slot_at):
        for t in range(3):
            source = slot_at * 3 + t
            total = [None] * SIZE
            for k in range(SIZE):
                column = routed[source, pl.ds(k, SIZE, stride=16), :]
                for a in range(SIZE):
                    term = routed[source, a * 16 + k : a * 16 + k + 1, :] * column
                    total[a] = term if k == 0 else total[a] + term
            for a in range(SIZE):
                packed[source, OFFSET[a] : OFFSET[a] + SIZE - a, :] = total[a][a:SIZE]
            packed[source, 0:1, :] = routed[source, 192:193, :]
            packed[source, 79:80, :] = routed[source, 192:193, :]

    def fill(target, index, part, tail):
        for begin, rows in CHUNKS:
            place = begin * 3 // 2
            target[index, place : place + rows, :] = packed[part, begin : begin + rows, :]
            half = rows // 2
            upper = packed[tail, begin : begin + half, :]
            bottom = packed[tail, begin + half : begin + rows, :]
            low = lanes((half, 128)) < 64
            if part == tail - 2:
                both = jnp.where(low, upper, pltpu.roll(bottom, 64, 1))
            else:
                both = jnp.where(low, pltpu.roll(upper, 64, 1), bottom)
            target[index, place + rows : place + rows + half, :] = both

    def copy1(i, chunk):
        begin, rows = CHUNKS[chunk]
        span = pl.ds(begin * 3 // 2, rows * 3 // 2)
        return pltpu.make_async_remote_copy(
            src_ref=send1.at[i, span],
            dst_ref=recv1.at[i, span],
            send_sem=sent.at[0],
            recv_sem=arrived.at[chunk * 2 + i // 4],
            device_id=partner1(i),
            device_id_type=MESH,
        )

    def pair(step, slot_at):
        multiply(slot_at)
        fill(recv1 if step == 0 else send1, 2 * step, slot_at * 3, slot_at * 3 + 2)
        fill(send1, 2 * step + 1, slot_at * 3 + 1, slot_at * 3 + 2)

    def start(step, chunk):
        if step:
            copy1(2 * step, chunk).start()
        copy1(2 * step + 1, chunk).start()

    route(1, 0)
    pair(1, 0)
    route(3, 1)
    pl.semaphore_wait(barrier, 11)
    start(1, 0)
    for target in near:
        pl.semaphore_signal(ready, inc=1, device_id=target, device_id_type=MESH)
    pair(3, 1)
    route(2, 0)
    start(3, 0)
    pair(2, 0)
    route(0, 1)
    start(2, 0)
    pair(0, 1)
    start(0, 0)
    for step in (1, 3, 2, 0):
        start(step, 1)
    pl.semaphore_wait(ready, 4)
    for target in next_near:
        pl.semaphore_signal(all_ready, inc=1, device_id=target, device_id_type=MESH)

    base = (lanes((1, 256)) & 15) * 16
    block = (lanes((1, 256)) & 63) >> 4
    low_row = lanes((1, 128)) < 64
    wanted = lax.broadcasted_iota(jnp.int32, (256, 256), 0)

    def batch(begin, chunk):
        first_row, rows = CHUNKS[chunk]
        at = first_row * 3 // 2
        low = lanes((rows // 2, 128)) < 64
        for delta in (2, 1, 3, 0):
            part = lax.rem(first // 2 + delta, 4)
            values = ids = None
            for source in range(4):
                i = begin + source
                half = recv1[i, at + rows : at + rows * 3 // 2, :]
                spread = jnp.concatenate(
                    [jnp.where(low, half, 0.0), jnp.where(low, 0.0, half)], axis=0
                )
                value = jnp.concatenate([recv1[i, at : at + rows, :], spread], axis=1)
                ids_half = recv1[i, 48:49, :]
                ids_half = jnp.where(low_row, ids_half, pltpu.roll(ids_half, 64, 1))
                ident = jnp.concatenate([recv1[i, 0:1, :], ids_half], axis=1)
                here = block == lax.rem(part + source, 4)
                values = value if source == 0 else jnp.where(here, value, values)
                ids = ident if source == 0 else jnp.where(here, ident, ids)
            place = base + ids.astype(jnp.int32)
            high = values.astype(BF16)
            rest = values - high.astype(F32)
            middle = rest.astype(BF16)
            tail = (rest - middle.astype(F32)).astype(BF16)
            pieces = jnp.concatenate([high, middle, tail], axis=0)
            choice = jnp.where(wanted == place, 1.0, 0.0).astype(BF16)
            found = lax.dot_general(
                pieces, choice, (((1,), (1,)), ((), ())), preferred_element_type=F32
            )
            found = found[0:rows] + found[rows : 2 * rows] + found[2 * rows : 3 * rows]
            for side in range(2):
                piece = found[:, side * 128 : side * 128 + 128]
                if begin:
                    piece = dense[2 * part + side, first_row : first_row + rows, :] + piece
                dense[2 * part + side, first_row : first_row + rows, :] = piece
            if begin and delta:
                copy2(2 * part, first, chunk).start()
                copy2(2 * part + 1, first, chunk).start()
            elif begin:
                copy2(first + 1 - 2 * lax.rem(first, 2), first, chunk).start()

    def copy2(target, source, chunk):
        begin, rows = CHUNKS[chunk]
        return pltpu.make_async_remote_copy(
            src_ref=dense.at[target, pl.ds(begin, rows)],
            dst_ref=recv2.at[source, pl.ds(begin, rows)],
            send_sem=sent.at[1],
            recv_sem=arrived.at[4 + chunk],
            device_id=device(
                target * core + y * (1 - core), x, core, z * core + target * (1 - core)
            ),
            device_id_type=MESH,
        )

    for chunk, (begin, rows) in enumerate(CHUNKS):
        part_rows = (begin * 3 // 2, rows * 3 // 2)
        wait_for(recv1, 1, 3, arrived.at[chunk * 2], part_rows)
        batch(0, chunk)
        wait_for(recv1, 4, 4, arrived.at[chunk * 2 + 1], part_rows)
        if chunk == 0:
            pl.semaphore_wait(all_ready, 4)
        batch(4, chunk)

    lane_full = lanes((8, 128))

    def swap(tiles):
        for span in (4, 2, 1):
            width = span * 16
            lower = (lane_full & width) == 0
            result = list(tiles)
            for v in range(8):
                if v & span:
                    continue
                one, two = tiles[v], tiles[v + span]
                result[v] = jnp.where(lower, one, pltpu.roll(two, width, 1))
                result[v + span] = jnp.where(lower, pltpu.roll(one, 128 - width, 1), two)
            tiles = result
        return tiles

    def copy3(i, chunk):
        return pltpu.make_async_remote_copy(
            src_ref=send3.at[lax.rem(second + i, 8), chunk],
            dst_ref=recv3.at[i, chunk],
            send_sem=sent.at[2],
            recv_sem=arrived.at[6],
            device_id=partner3(i),
            device_id_type=MESH,
        )

    empty = jnp.zeros((8, 128), F32)
    for chunk, (begin, rows) in enumerate(CHUNKS):
        wait_for(recv2, 0, 7, arrived.at[4 + chunk], (begin, rows))
        total = dense[first, begin : begin + rows, :]
        for i in range(1, 8):
            total = total + recv2[lax.rem(first + i, 8), begin : begin + rows, :]
        tiles = [total[v * 8 : v * 8 + 8] for v in range(rows // 8)]
        tiles = swap(tiles + [empty] * (8 - len(tiles)))
        for q in range(8):
            send3[q, chunk] = tiles[q]
        for i in (4, 3, 5, 2, 6, 1, 7):
            copy3(i, chunk).start()
    wait_for(recv3, 1, 7, arrived.at[6])
    for chunk in range(2):
        result = send3[second, chunk]
        for i in range(1, 8):
            result = result + recv3[i, chunk]
        out[chunk * 8 : chunk * 8 + 8, :] = result
    wait_for(recv1, 1, 7, sent.at[0])
    wait_for(recv2, 0, 7, sent.at[1])
    wait_for(recv3, 1, 7, sent.at[2])


def inverse_kernel(sums, shift, out, flat, square):
    for v in range(10):
        source = sums[0:8, :] if v < 6 else sums[8:16, :]
        turned = 16 * (v if v < 6 else v - 6)
        flat[v * 8 : v * 8 + 8, :] = pltpu.roll(source, 128 - turned, 1) if turned else source
    for j in range(SIZE):
        square[j, j:SIZE, :] = flat[OFFSET[j] : OFFSET[j] + SIZE - j, 0:NODES]
        for i in range(j):
            place = OFFSET[i] + j - i
            square[j, i : i + 1, :] = flat[place : place + 1, 0:NODES]
    row = lax.broadcasted_iota(jnp.int32, (SIZE, NODES), 0)
    columns = []
    for j in range(SIZE):
        added = jnp.where(row == j, shift[j : j + 1, :], 0.0)
        columns.append(square[j] + added)
    for j in range(SIZE):
        current = columns[j]
        here = row == j
        scale = 1.0 / current[j : j + 1, :]
        scaled = jnp.where(here, -scale, current * scale)
        for k in range(SIZE):
            if k == j:
                continue
            kept = jnp.where(here, 0.0, columns[k])
            columns[k] = kept - scaled * current[k : k + 1, :]
        columns[j] = scaled
    for j in range(SIZE):
        out[j] = -columns[j]


def shards(factors, dest_device, dest_node, live_count, shift):
    vmem = pl.BlockSpec(memory_space=pltpu.VMEM)
    in_hbm = functools.partial(pltpu.with_memory_space_constraint, memory_space=pltpu.HBM)
    sums = pl.pallas_call(
        exchange_kernel,
        out_shape=jax.ShapeDtypeStruct((16, 128), F32),
        in_specs=[pl.BlockSpec(memory_space=pltpu.HBM)] * 3
        + [pl.BlockSpec(memory_space=pltpu.SMEM)],
        out_specs=vmem,
        scratch_shapes=[
            pltpu.VMEM((SIZE, SIZE, COUNT), BF16),
            pltpu.VMEM((1, COUNT), jnp.int32),
            pltpu.VMEM((1, COUNT), jnp.int32),
            pltpu.SemaphoreType.DMA((3,)),
            pltpu.VMEM((208, COUNT), BF16),
            pltpu.VMEM((6, 208, 128), F32),
            pltpu.VMEM((6, ROWS, 128), F32),
            pltpu.VMEM((8, MESSAGE, 128), F32),
            pltpu.VMEM((8, MESSAGE, 128), F32),
            pltpu.VMEM((8, ROWS, 128), F32),
            pltpu.VMEM((8, ROWS, 128), F32),
            pltpu.VMEM((8, 2, 8, 128), F32),
            pltpu.VMEM((8, 2, 8, 128), F32),
        ]
        + [pltpu.SemaphoreType.DMA((3,)), pltpu.SemaphoreType.DMA((7,))]
        + [pltpu.SemaphoreType.REGULAR] * 2,
        compiler_params=pltpu.CompilerParams(
            collective_id=0, has_side_effects=True, vmem_limit_bytes=16 << 20
        ),
    )(
        in_hbm(factors),
        in_hbm(dest_device.reshape(1, COUNT)),
        in_hbm(dest_node.reshape(1, COUNT)),
        live_count,
    )
    return pl.pallas_call(
        inverse_kernel,
        out_shape=jax.ShapeDtypeStruct((SIZE, SIZE, NODES), F32),
        in_specs=[vmem, vmem],
        out_specs=vmem,
        scratch_shapes=[pltpu.VMEM((ROWS, 128), F32), pltpu.VMEM((SIZE, SIZE, NODES), F32)],
        compiler_params=pltpu.CompilerParams(vmem_limit_bytes=4 << 20),
    )(sums, shift)


def solution(mesh):
    placed = (
        P(None, None, ("elem", "node")),
        P(("elem", "node"), None),
        P(("elem", "node"), None),
        P(("elem", "node")),
        P(None, ("elem", "node")),
    )
    return jax.shard_map(
        shards,
        mesh=mesh,
        in_specs=placed,
        out_specs=P(None, None, ("elem", "node")),
        check_vma=False,
    )
```

```python
import functools

import jax
import jax.numpy as jnp
from jax import lax
from jax.experimental import pallas as pl
from jax.experimental.pallas import tpu as pltpu
from jax.sharding import PartitionSpec as P

MESH = pl.DeviceIdType.MESH
F32 = jnp.float32
BF16 = jnp.bfloat16
SIZE = 12
COUNT = 1024
NODES = 16
NX, NY, NZ, NC = 4, 8, 8, 2
OFFSET = [1 + a * SIZE - a * (a - 1) // 2 for a in range(SIZE)]
ROWS = 80
MESSAGE = 120
CHUNKS = ((0, 48), (48, 32))


def lanes(shape):
    return lax.broadcasted_iota(jnp.int32, shape, len(shape) - 1)


def ranks_of(owner):
    counts = [jnp.zeros((8, 128), F32) for _ in range(8)]
    rows = [owner[:, b * 128 : (b + 1) * 128] for b in range(8)]
    before = lax.broadcasted_iota(jnp.int32, (128, 128), 0) < lanes((128, 128))
    for b in range(8):
        column = jnp.broadcast_to(rows[b], (128, 128)).T
        for later in range(b, 8):
            same = column == rows[later]
            if later == b:
                same = same & before
            hits = jnp.where(same, 1.0, 0.0)
            counts[later] = counts[later] + jnp.sum(hits.reshape(16, 8, 128), axis=0)
    return jnp.concatenate([jnp.sum(c, axis=0, keepdims=True) for c in counts], axis=1)


def wait_for(buffer, begin, count, semaphore, rows=None):
    span = buffer.at[pl.ds(begin, count)]
    if rows is not None:
        span = buffer.at[pl.ds(begin, count), pl.ds(*rows)]
    pltpu.make_async_copy(span, span, semaphore).wait()


def exchange_kernel(
    factors_in,
    owner_in,
    node_in,
    live_ref,
    out,
    factors,
    owner_ref,
    node_ref,
    isem,
    lhs,
    routed,
    packed,
    send1,
    recv1,
    dense,
    recv2,
    send3,
    recv3,
    sent,
    arrived,
    ready,
    all_ready,
):
    inputs = [
        pltpu.make_async_copy(source, target, isem.at[n])
        for n, (source, target) in enumerate(
            [(owner_in, owner_ref), (node_in, node_ref), (factors_in, factors)]
        )
    ]
    for copy in inputs:
        copy.start()
    elem = lax.axis_index("elem")
    z = lax.axis_index("node")
    core = lax.rem(elem, NC)
    x = lax.rem(elem // NC, NX)
    y = elem // (NC * NX)

    def device(y_at, x_at, core_at, z_at):
        return ((y_at * NX + x_at) * NC + core_at, z_at)

    def partner1(i):
        return device(y, lax.rem(x + i // 2, NX), lax.rem(core + i, NC), z)

    def partner2(i):
        return device(lax.rem(y + i * core, NY), x, core, lax.rem(z + i * (1 - core), NZ))

    def partner3(i):
        return device(lax.rem(y + i * (1 - core), NY), x, core, lax.rem(z + i * core, NZ))

    barrier = pltpu.get_barrier_semaphore()
    near = [partner(i) for partner in (partner2, partner3) for i in (1, 7)]
    next_near = [partner(i) for partner in (partner2, partner3) for i in (2, 6)]
    for target in near + [partner1(i) for i in range(1, 8)]:
        pl.semaphore_signal(barrier, inc=1, device_id=target, device_id_type=MESH)

    first = y * core + z * (1 - core)
    second = z * core + y * (1 - core)

    inputs[0].wait()
    owner = owner_ref[...]
    rank = ranks_of(owner.astype(F32)).astype(jnp.int32)
    owner_z = owner & 7
    owner_core = (owner >> 3) & 1
    owner_x = (owner >> 4) & 3
    owner_y = owner >> 6
    other = owner_core ^ core
    step = (owner_x - x + NX) & 3
    slot = jnp.where(rank < 2, other * 128 + rank * 64, 256 + other * 64)
    outer = owner_y * owner_core + owner_z * (1 - owner_core)
    inner = owner_z * owner_core + owner_y * (1 - owner_core)
    lane = (outer * 8 + inner + ((2 * step + other) & 3) * 16) & 63
    slot = slot + step * 384 + lane
    slot = jnp.where(lanes((1, COUNT)) < live_ref[0], slot, -1)

    inputs[1].wait()
    inputs[2].wait()
    for a in range(SIZE):
        lhs[a * 16 : a * 16 + SIZE, :] = factors[a]
    lhs[192:208, :] = jnp.broadcast_to(node_ref[...].astype(F32), (16, COUNT)).astype(BF16)

    def route(step, slot_at):
        wanted = lax.broadcasted_iota(jnp.int32, (384, COUNT), 0)
        choice = jnp.where(wanted == slot - step * 384, 1.0, 0.0).astype(BF16)
        result = lax.dot_general(
            lhs[...], choice, (((1,), (1,)), ((), ())), preferred_element_type=F32
        )
        for t in range(3):
            routed[slot_at * 3 + t] = result[:, t * 128 : (t + 1) * 128]

    def multiply(slot_at):
        for t in range(3):
            source = slot_at * 3 + t
            total = [None] * SIZE
            for k in range(SIZE):
                column = routed[source, pl.ds(k, SIZE, stride=16), :]
                for a in range(SIZE):
                    term = routed[source, a * 16 + k : a * 16 + k + 1, :] * column
                    total[a] = term if k == 0 else total[a] + term
            for a in range(SIZE):
                packed[source, OFFSET[a] : OFFSET[a] + SIZE - a, :] = total[a][a:SIZE]
            packed[source, 0:1, :] = routed[source, 192:193, :]
            packed[source, 79:80, :] = routed[source, 192:193, :]

    def fill(target, index, part, tail):
        for begin, rows in CHUNKS:
            place = begin * 3 // 2
            target[index, place : place + rows, :] = packed[part, begin : begin + rows, :]
            half = rows // 2
            upper = packed[tail, begin : begin + half, :]
            bottom = packed[tail, begin + half : begin + rows, :]
            low = lanes((half, 128)) < 64
            if part == tail - 2:
                both = jnp.where(low, upper, pltpu.roll(bottom, 64, 1))
            else:
                both = jnp.where(low, pltpu.roll(upper, 64, 1), bottom)
            target[index, place + rows : place + rows + half, :] = both

    def copy1(i, chunk):
        begin, rows = CHUNKS[chunk]
        span = pl.ds(begin * 3 // 2, rows * 3 // 2)
        return pltpu.make_async_remote_copy(
            src_ref=send1.at[i, span],
            dst_ref=recv1.at[i, span],
            send_sem=sent.at[0],
            recv_sem=arrived.at[chunk * 2 + i // 4],
            device_id=partner1(i),
            device_id_type=MESH,
        )

    def pair(step, slot_at):
        multiply(slot_at)
        fill(recv1 if step == 0 else send1, 2 * step, slot_at * 3, slot_at * 3 + 2)
        fill(send1, 2 * step + 1, slot_at * 3 + 1, slot_at * 3 + 2)

    def start(step, chunk):
        if step:
            copy1(2 * step, chunk).start()
        copy1(2 * step + 1, chunk).start()

    route(1, 0)
    pair(1, 0)
    route(3, 1)
    pl.semaphore_wait(barrier, 11)
    start(1, 0)
    for target in near:
        pl.semaphore_signal(ready, inc=1, device_id=target, device_id_type=MESH)
    pair(3, 1)
    route(2, 0)
    start(3, 0)
    pair(2, 0)
    start(2, 0)
    route(0, 1)
    pair(0, 1)
    start(0, 0)
    for step in (1, 3, 2, 0):
        start(step, 1)
    pl.semaphore_wait(ready, 4)
    for target in next_near:
        pl.semaphore_signal(all_ready, inc=1, device_id=target, device_id_type=MESH)

    base = (lanes((1, 256)) & 15) * 16
    block = (lanes((1, 256)) & 63) >> 4
    low_row = lanes((1, 128)) < 64
    wanted = lax.broadcasted_iota(jnp.int32, (256, 256), 0)

    def batch(begin, chunk):
        first_row, rows = CHUNKS[chunk]
        at = first_row * 3 // 2
        low = lanes((rows // 2, 128)) < 64
        for delta in (2, 1, 3, 0):
            part = lax.rem(first // 2 + delta, 4)
            values = ids = None
            for source in range(4):
                i = begin + source
                half = recv1[i, at + rows : at + rows * 3 // 2, :]
                spread = jnp.concatenate(
                    [jnp.where(low, half, 0.0), jnp.where(low, 0.0, half)], axis=0
                )
                value = jnp.concatenate([recv1[i, at : at + rows, :], spread], axis=1)
                ids_half = recv1[i, 48:49, :]
                ids_half = jnp.where(low_row, ids_half, pltpu.roll(ids_half, 64, 1))
                ident = jnp.concatenate([recv1[i, 0:1, :], ids_half], axis=1)
                here = block == lax.rem(part + source, 4)
                values = value if source == 0 else jnp.where(here, value, values)
                ids = ident if source == 0 else jnp.where(here, ident, ids)
            place = base + ids.astype(jnp.int32)
            high = values.astype(BF16)
            rest = values - high.astype(F32)
            middle = rest.astype(BF16)
            tail = (rest - middle.astype(F32)).astype(BF16)
            pieces = jnp.concatenate([high, middle, tail], axis=0)
            choice = jnp.where(wanted == place, 1.0, 0.0).astype(BF16)
            found = lax.dot_general(
                pieces, choice, (((1,), (1,)), ((), ())), preferred_element_type=F32
            )
            found = found[0:rows] + found[rows : 2 * rows] + found[2 * rows : 3 * rows]
            for side in range(2):
                piece = found[:, side * 128 : side * 128 + 128]
                if begin:
                    piece = dense[2 * part + side, first_row : first_row + rows, :] + piece
                dense[2 * part + side, first_row : first_row + rows, :] = piece
            if begin and delta:
                copy2(2 * part, first, chunk).start()
                copy2(2 * part + 1, first, chunk).start()
            elif begin:
                copy2(first + 1 - 2 * lax.rem(first, 2), first, chunk).start()

    def copy2(target, source, chunk):
        begin, rows = CHUNKS[chunk]
        return pltpu.make_async_remote_copy(
            src_ref=dense.at[target, pl.ds(begin, rows)],
            dst_ref=recv2.at[source, pl.ds(begin, rows)],
            send_sem=sent.at[1],
            recv_sem=arrived.at[4 + chunk],
            device_id=device(
                target * core + y * (1 - core), x, core, z * core + target * (1 - core)
            ),
            device_id_type=MESH,
        )

    for chunk, (begin, rows) in enumerate(CHUNKS):
        part_rows = (begin * 3 // 2, rows * 3 // 2)
        wait_for(recv1, 1, 3, arrived.at[chunk * 2], part_rows)
        batch(0, chunk)
        wait_for(recv1, 4, 4, arrived.at[chunk * 2 + 1], part_rows)
        if chunk == 0:
            pl.semaphore_wait(all_ready, 4)
        batch(4, chunk)

    lane_full = lanes((8, 128))

    def swap(tiles):
        for span in (4, 2, 1):
            width = span * 16
            lower = (lane_full & width) == 0
            result = list(tiles)
            for v in range(8):
                if v & span:
                    continue
                one, two = tiles[v], tiles[v + span]
                result[v] = jnp.where(lower, one, pltpu.roll(two, width, 1))
                result[v + span] = jnp.where(lower, pltpu.roll(one, 128 - width, 1), two)
            tiles = result
        return tiles

    def copy3(i, chunk):
        return pltpu.make_async_remote_copy(
            src_ref=send3.at[lax.rem(second + i, 8), chunk],
            dst_ref=recv3.at[i, chunk],
            send_sem=sent.at[2],
            recv_sem=arrived.at[6],
            device_id=partner3(i),
            device_id_type=MESH,
        )

    empty = jnp.zeros((8, 128), F32)
    for chunk, (begin, rows) in enumerate(CHUNKS):
        wait_for(recv2, 0, 7, arrived.at[4 + chunk], (begin, rows))
        total = dense[first, begin : begin + rows, :]
        for i in range(1, 8):
            total = total + recv2[lax.rem(first + i, 8), begin : begin + rows, :]
        tiles = [total[v * 8 : v * 8 + 8] for v in range(rows // 8)]
        tiles = swap(tiles + [empty] * (8 - len(tiles)))
        for q in range(8):
            send3[q, chunk] = tiles[q]
        for i in (4, 3, 5, 2, 6, 1, 7):
            copy3(i, chunk).start()
    wait_for(recv3, 1, 7, arrived.at[6])
    for chunk in range(2):
        result = send3[second, chunk]
        for i in range(1, 8):
            result = result + recv3[i, chunk]
        out[chunk * 8 : chunk * 8 + 8, :] = result
    wait_for(recv1, 1, 7, sent.at[0])
    wait_for(recv2, 0, 7, sent.at[1])
    wait_for(recv3, 1, 7, sent.at[2])


def inverse_kernel(sums, shift, out, flat, square):
    for v in range(10):
        source = sums[0:8, :] if v < 6 else sums[8:16, :]
        turned = 16 * (v if v < 6 else v - 6)
        flat[v * 8 : v * 8 + 8, :] = pltpu.roll(source, 128 - turned, 1) if turned else source
    for j in range(SIZE):
        square[j, j:SIZE, :] = flat[OFFSET[j] : OFFSET[j] + SIZE - j, 0:NODES]
        for i in range(j):
            place = OFFSET[i] + j - i
            square[j, i : i + 1, :] = flat[place : place + 1, 0:NODES]
    row = lax.broadcasted_iota(jnp.int32, (SIZE, NODES), 0)
    columns = []
    for j in range(SIZE):
        added = jnp.where(row == j, shift[j : j + 1, :], 0.0)
        columns.append(square[j] + added)
    for j in range(SIZE):
        current = columns[j]
        here = row == j
        scale = 1.0 / current[j : j + 1, :]
        scaled = jnp.where(here, -scale, current * scale)
        for k in range(SIZE):
            if k == j:
                continue
            kept = jnp.where(here, 0.0, columns[k])
            columns[k] = kept - scaled * current[k : k + 1, :]
        columns[j] = scaled
    for j in range(SIZE):
        out[j] = -columns[j]


def shards(factors, dest_device, dest_node, live_count, shift):
    vmem = pl.BlockSpec(memory_space=pltpu.VMEM)
    in_hbm = functools.partial(pltpu.with_memory_space_constraint, memory_space=pltpu.HBM)
    sums = pl.pallas_call(
        exchange_kernel,
        out_shape=jax.ShapeDtypeStruct((16, 128), F32),
        in_specs=[pl.BlockSpec(memory_space=pltpu.HBM)] * 3
        + [pl.BlockSpec(memory_space=pltpu.SMEM)],
        out_specs=vmem,
        scratch_shapes=[
            pltpu.VMEM((SIZE, SIZE, COUNT), BF16),
            pltpu.VMEM((1, COUNT), jnp.int32),
            pltpu.VMEM((1, COUNT), jnp.int32),
            pltpu.SemaphoreType.DMA((3,)),
            pltpu.VMEM((208, COUNT), BF16),
            pltpu.VMEM((6, 208, 128), F32),
            pltpu.VMEM((6, ROWS, 128), F32),
            pltpu.VMEM((8, MESSAGE, 128), F32),
            pltpu.VMEM((8, MESSAGE, 128), F32),
            pltpu.VMEM((8, ROWS, 128), F32),
            pltpu.VMEM((8, ROWS, 128), F32),
            pltpu.VMEM((8, 2, 8, 128), F32),
            pltpu.VMEM((8, 2, 8, 128), F32),
        ]
        + [pltpu.SemaphoreType.DMA((3,)), pltpu.SemaphoreType.DMA((7,))]
        + [pltpu.SemaphoreType.REGULAR] * 2,
        compiler_params=pltpu.CompilerParams(
            collective_id=0, has_side_effects=True, vmem_limit_bytes=16 << 20
        ),
    )(
        in_hbm(factors),
        in_hbm(dest_device.reshape(1, COUNT)),
        in_hbm(dest_node.reshape(1, COUNT)),
        live_count,
    )
    return pl.pallas_call(
        inverse_kernel,
        out_shape=jax.ShapeDtypeStruct((SIZE, SIZE, NODES), F32),
        in_specs=[vmem, vmem],
        out_specs=vmem,
        scratch_shapes=[pltpu.VMEM((ROWS, 128), F32), pltpu.VMEM((SIZE, SIZE, NODES), F32)],
        compiler_params=pltpu.CompilerParams(vmem_limit_bytes=4 << 20),
    )(sums, shift)


def solution(mesh):
    placed = (
        P(None, None, ("elem", "node")),
        P(("elem", "node"), None),
        P(("elem", "node"), None),
        P(("elem", "node")),
        P(None, ("elem", "node")),
    )
    return jax.shard_map(
        shards,
        mesh=mesh,
        in_specs=placed,
        out_specs=P(None, None, ("elem", "node")),
        check_vma=False,
    )
```
